32 devices in a mesh: dp: 1 (over z), cp: 32 (over y, x, core).
Axes of the slice: x: 4, y: 4, z: 1, core: 2. Of those that a mesh axis runs over, the one named last changes fastest.
The devices are a block of a 4x4x8 slice.
Arguments:
- q_tokens: bfloat16 [2048, 12, 128], P(('dp', 'cp'))
- k_tokens: bfloat16 [2048, 2, 128], P(('dp', 'cp'))
- v_tokens: bfloat16 [2048, 2, 128], P(('dp', 'cp'))
- d_out: bfloat16 [2048, 12, 128], P(('dp', 'cp'))
- key_valid: int32 [2048], P(('dp', 'cp'))
- cu_seqlens: int32 [3], P('dp')
Outputs:
- output 1: bfloat16 [2048, 12, 128], P(('dp', 'cp'))
- output 2: float32 [2048, 12], P(('dp', 'cp'))
- output 3: bfloat16 [2048, 12, 128], P(('dp', 'cp'))
- output 4: bfloat16 [2048, 2, 128], P(('dp', 'cp'))
- output 5: bfloat16 [2048, 2, 128], P(('dp', 'cp'))
All inputs are finite; a program needn't handle non-finite values.
Results may differ from the reference program's by a relative error of at most 0.00866085.
Values are sent between devices in bfloat16 or wider.
A program may use at most 768 MiB of HBM per device.

```python
import jax
import jax.numpy as jnp
from jax import lax

HEADS = 12
KV_HEADS = 2
HEAD = 128
TOK_DEV = 64
DOCS = 2
CP = 32
TOKENS = TOK_DEV * CP
GROUP = HEADS // KV_HEADS
Q_BLOCK = min(32, TOKENS)
MASK_FILL = -1.0e30


def token_coords(cu_seqlens, rank_ids, local_ids):
    starts = cu_seqlens[:-1] // CP
    doc_id = jnp.sum((local_ids[..., None] >= starts).astype(jnp.int32), axis=-1) - 1
    seg_start = cu_seqlens[doc_id]
    piece_len = (cu_seqlens[doc_id + 1] - seg_start) // (2 * CP)
    within = local_ids - seg_start // CP
    in_upper = (within >= piece_len).astype(jnp.int32)
    piece_idx = rank_ids + in_upper * (2 * CP - 1 - 2 * rank_ids)
    position = seg_start + piece_idx * piece_len + within - in_upper * piece_len
    return doc_id, position


def draw_layout(layout_key):
    key_cut, key_pad = jax.random.split(layout_key)
    unit_count = TOKENS // (2 * CP)
    cut_points = jnp.sort(jax.random.permutation(key_cut, unit_count - 1)[:DOCS - 1] + 1)
    bounds = jnp.concatenate([jnp.zeros((1,), jnp.int32), cut_points.astype(jnp.int32), jnp.full((1,), unit_count, jnp.int32)]) * (2 * CP)
    pad_len = jax.random.randint(key_pad, (DOCS,), 0, 2 * CP)
    tok_index = jnp.arange(TOKENS)
    doc_id, position = token_coords(bounds, tok_index // TOK_DEV, tok_index % TOK_DEV)
    key_valid = (position < bounds[doc_id + 1] - pad_len[doc_id]).astype(jnp.int32)
    return bounds, key_valid


def setup_inputs(seed: int = 0, part: int = 0) -> dict:
    part_key = jax.random.fold_in(jax.random.key(seed), part)
    key_list = jax.random.split(part_key, 5)
    cu_seqlens, key_valid = draw_layout(key_list[0])
    q_tokens = jax.random.normal(key_list[1], (TOKENS, HEADS, HEAD), jnp.float32).astype(jnp.bfloat16)
    k_tokens = jax.random.normal(key_list[2], (TOKENS, KV_HEADS, HEAD), jnp.float32).astype(jnp.bfloat16)
    v_tokens = jax.random.normal(key_list[3], (TOKENS, KV_HEADS, HEAD), jnp.float32).astype(jnp.bfloat16)
    d_out = jax.random.normal(key_list[4], (TOKENS, HEADS, HEAD), jnp.float32).astype(jnp.bfloat16)
    return {'q_tokens': q_tokens, 'k_tokens': k_tokens, 'v_tokens': v_tokens, 'd_out': d_out, 'key_valid': key_valid, 'cu_seqlens': cu_seqlens}


def reference(q_tokens, k_tokens, v_tokens, d_out, key_valid, cu_seqlens):
    tok_index = jnp.arange(TOKENS)
    doc_id, position = token_coords(cu_seqlens, tok_index // TOK_DEV, tok_index % TOK_DEV)
    key_ok = key_valid > 0
    score_scale = HEAD ** -0.5
    k_full = k_tokens.astype(jnp.float32)
    v_full = v_tokens.astype(jnp.float32)
    n_blocks = TOKENS // Q_BLOCK
    q_blocks = q_tokens.reshape(n_blocks, Q_BLOCK, KV_HEADS, GROUP, HEAD)
    do_blocks = d_out.reshape(n_blocks, Q_BLOCK, KV_HEADS, GROUP, HEAD)
    doc_blocks = doc_id.reshape(n_blocks, Q_BLOCK)
    pos_blocks = position.reshape(n_blocks, Q_BLOCK)

    def block_scores(q_blk, doc_q, pos_q):
        scores = jnp.einsum('qhgd,khd->hgqk', q_blk.astype(jnp.float32), k_full) * score_scale
        allowed = (doc_q[:, None] == doc_id[None, :]) & (position[None, :] <= pos_q[:, None]) & key_ok[None, :]
        return jnp.where(allowed, scores, MASK_FILL), allowed

    def forward_block(inputs):
        q_blk, doc_q, pos_q = inputs
        scores, allowed = block_scores(q_blk, doc_q, pos_q)
        row_max = jnp.max(scores, axis=-1)
        weights = jnp.where(allowed, jnp.exp(scores - row_max[..., None]), 0.0)
        row_sum = jnp.sum(weights, axis=-1)
        has_key = row_sum > 0
        safe_den = jnp.where(has_key, row_sum, 1.0)
        acc_out = jnp.einsum('hgqk,khd->qhgd', weights, v_full)
        inv_den = jnp.where(has_key, 1.0 / safe_den, 0.0)
        out_blk = acc_out * jnp.transpose(inv_den, (2, 0, 1))[..., None]
        lse_blk = jnp.where(has_key, row_max + jnp.log(safe_den), 0.0)
        return out_blk.astype(jnp.bfloat16), jnp.transpose(lse_blk, (2, 0, 1))

    out_blocks, lse_blocks = lax.map(forward_block, (q_blocks, doc_blocks, pos_blocks))

    def backward_block(grad_acc, inputs):
        dk_acc, dv_acc = grad_acc
        q_blk, do_blk, out_blk, lse_blk, doc_q, pos_q = inputs
        scores, allowed = block_scores(q_blk, doc_q, pos_q)
        lse_hgq = jnp.transpose(lse_blk, (1, 2, 0))
        weights = jnp.where(allowed, jnp.exp(scores - lse_hgq[..., None]), 0.0)
        do_full = do_blk.astype(jnp.float32)
        row_delta = jnp.transpose(jnp.sum(do_full * out_blk.astype(jnp.float32), axis=-1), (1, 2, 0))
        d_prob = jnp.einsum('qhgd,khd->hgqk', do_full, v_full)
        d_score = weights * (d_prob - row_delta[..., None])
        dq_blk = jnp.einsum('hgqk,khd->qhgd', d_score, k_full) * score_scale
        dk_acc = dk_acc + jnp.einsum('hgqk,qhgd->khd', d_score, q_blk.astype(jnp.float32)) * score_scale
        dv_acc = dv_acc + jnp.einsum('hgqk,qhgd->khd', weights, do_full)
        return (dk_acc, dv_acc), dq_blk.astype(jnp.bfloat16)

    zero_acc = jnp.zeros((TOKENS, KV_HEADS, HEAD), jnp.float32)
    grad_sums, dq_blocks = lax.scan(backward_block, (zero_acc, zero_acc), (q_blocks, do_blocks, out_blocks, lse_blocks, doc_blocks, pos_blocks))
    attn_out = out_blocks.reshape(TOKENS, HEADS, HEAD)
    log_sumexp = lse_blocks.reshape(TOKENS, HEADS)
    d_query = dq_blocks.reshape(TOKENS, HEADS, HEAD)
    return attn_out, log_sumexp, d_query, grad_sums[0].astype(jnp.bfloat16), grad_sums[1].astype(jnp.bfloat16)
```

```python
import functools
import math

import jax
import jax.numpy as jnp
from jax import lax
from jax.experimental import pallas as pl
from jax.experimental.pallas import tpu as pltpu
from jax.sharding import PartitionSpec as P

MESH = pl.DeviceIdType.MESH
NEG = -(2.0 ** 126)
CORES = 2
SIDE = 4
LEVELS = (
    ((0, 0),),
    ((1, 0), (3, 0), (0, 1), (0, 3)),
    ((2, 0), (0, 2), (1, 1), (1, 3), (3, 1), (3, 3)),
    ((2, 1), (2, 3), (1, 2), (3, 2)),
    ((2, 2),),
)
BLOCKS = tuple(blk for level in LEVELS for blk in level)
SLOT = {blk: i for i, blk in enumerate(BLOCKS)}
NBLK = len(BLOCKS)
NT = (((1,), (1,)), ((), ()))
TN = (((0,), (0,)), ((), ()))


def dot(a, b, dims=(((1,), (0,)), ((), ()))):
    return lax.dot_general(a, b, dims, preferred_element_type=jnp.float32)


def frame(X, blk):
    return blk if X == 0 else (blk[1], blk[0])


def unframe(X, a, b):
    return (a, b) if X == 0 else (b, a)


def routes(X, blk, o):
    a, b = frame(X, blk)
    out = []
    if b == 0:
        if a == 3 and o == 0:
            out.append((1, 0))
        if a == 1 and o == 1:
            out.append((-1, 0))
        if a == 0:
            out += [(1, 0), (-1, 0)]
        out += [(0, 1), (0, -1)]
    elif b == 3 and o == 0:
        out.append((0, 1))
    elif b == 1 and o == 1:
        out.append((0, -1))
    return [unframe(X, *step) for step in out]


RKEYS = []
for _a in range(SIDE):
    RKEYS += [('rb', _a, 0), ('rb', _a, 1)]
    RKEYS += [('fb', _a, _o, _s) for _o in range(2) for _s in (1, -1)]
RKEYS += [('ra', 0), ('ra', 1)]
RKEYS += [('fa', _o, _s) for _o in range(2) for _s in (1, -1)]
RIDX = {key: i for i, key in enumerate(RKEYS)}


def kernel(cp, n_docs, scale, q_hbm, k_hbm, v_hbm, do_hbm, val_hbm, cu_hbm,
           o_hbm, lse_hbm, dq_hbm, dk_hbm, dv_hbm,
           kin, kf32, oth, kv, kaug, qaug, dob, dot_t, sbuf, dpbuf, pbuf, dsbuf, part, rbuf,
           ost, dqst, lsest, kvsend, kvrecv, tmp32, outb, m_ref, l_ref, o_t, valv, cus,
           loc_sem, pair_send, pair_recv, ag_send, ag_recv, rs_send, rs_recv):
    tok = valv.shape[1]
    grp = ost.shape[0] // CORES
    rows = CORES * grp * tok
    hd = kin.shape[-1]
    keys = CORES * tok
    me = lax.axis_index('cp')
    core = lax.rem(me, CORES)
    chip = lax.div(me, CORES)
    cx = lax.rem(chip, SIDE)
    cy = lax.div(chip, SIDE)
    partner = me + 1 - 2 * core

    def chip_at(dx, dy):
        return lax.rem(cy + dy + SIDE, SIDE) * SIDE + lax.rem(cx + dx + SIDE, SIDE)

    def nbr(step):
        return {'cp': chip_at(*step) * CORES + core}

    mine = core * grp
    theirs = (1 - core) * grp
    to_partner = {'cp': partner}

    c_k = pltpu.make_async_copy(k_hbm, kin.at[0], loc_sem.at[0])
    c_v = pltpu.make_async_copy(v_hbm, kin.at[1], loc_sem.at[1])
    c_val = pltpu.make_async_copy(val_hbm, valv, loc_sem.at[2])
    c_cu = pltpu.make_async_copy(cu_hbm, cus, loc_sem.at[3])
    c_q = pltpu.make_async_copy(q_hbm.at[pl.ds(mine, grp)], qaug.at[0:grp, :, 0:hd], loc_sem.at[4])
    c_do = pltpu.make_async_copy(do_hbm.at[pl.ds(mine, grp)], dob.at[0:grp], loc_sem.at[5])
    for c in (c_k, c_v, c_val, c_cu, c_q, c_do):
        c.start()

    barrier = pltpu.get_barrier_semaphore()
    peers = [to_partner] + [nbr(s) for s in ((1, 0), (-1, 0), (0, 1), (0, -1))]
    for peer in peers:
        pl.semaphore_signal(barrier, inc=1, device_id=peer, device_id_type=MESH)

    sends = []

    def remote(src, dst, ssem, rsem, dev):
        copy = pltpu.make_async_remote_copy(src_ref=src, dst_ref=dst, send_sem=ssem, recv_sem=rsem,
                                            device_id=dev, device_id_type=MESH)
        return copy

    def push(src, dst, ssem, rsem, dev):
        copy = remote(src, dst, ssem, rsem, dev)
        copy.start()
        sends.append(copy)
        return copy

    for c in (c_k, c_v, c_val):
        c.wait()
    sub = lax.broadcasted_iota(jnp.int32, (tok, tok), 0)
    lane = lax.broadcasted_iota(jnp.int32, (tok, tok), 1)
    vcol = jnp.sum(jnp.where(sub == lane, jnp.broadcast_to(valv[...], (tok, tok)), 0), axis=1, keepdims=True)
    lane0 = lax.broadcasted_iota(jnp.int32, (tok, hd), 1) == 0
    bad = lane0 & (jnp.broadcast_to(vcol, (tok, hd)) <= 0)
    for X in range(2):
        kf32[X] = kin[X].astype(jnp.float32)
    for X in range(2):
        h0 = kf32[X, pl.ds(0, tok, stride=2), :]
        h1 = kf32[X, pl.ds(1, tok, stride=2), :]
        own = jnp.where(core == 0, h0, h1)
        other = jnp.where(core == 0, h1, h0)
        if X == 0:
            own = jnp.where(bad, jnp.inf, own)
            other = jnp.where(bad, jnp.inf, other)
        kv[X, 0, 0] = own.astype(jnp.bfloat16)
        oth[X] = other.astype(jnp.bfloat16)

    pl.semaphore_wait(barrier, len(peers))

    ag_count = [0]

    def forward(X, blk, o):
        for step in routes(X, blk, o):
            dst_blk = ((blk[0] - step[0]) % SIDE, (blk[1] - step[1]) % SIDE)
            s = SLOT[dst_blk]
            push(kv.at[X, SLOT[blk], o], kv.at[X, s, o], ag_send.at[ag_count[0]], ag_recv.at[X, s, o], nbr(step))
            ag_count[0] += 1

    def arrive(X, blk, o):
        s = SLOT[blk]
        remote(kv.at[X, s, o], kv.at[X, s, o], ag_send.at[0], ag_recv.at[X, s, o], to_partner).wait_recv()

    for X in range(2):
        push(oth.at[X], kv.at[X, 0, 1], pair_send.at[X], ag_recv.at[X, 0, 1], to_partner)
    for X in range(2):
        forward(X, (0, 0), 0)
    x_q = push(q_hbm.at[pl.ds(theirs, grp)], qaug.at[grp:2 * grp, :, 0:hd], pair_send.at[2], pair_recv.at[2], to_partner)
    x_do = push(do_hbm.at[pl.ds(theirs, grp)], dob.at[grp:2 * grp], pair_send.at[3], pair_recv.at[3], to_partner)

    t_row = lax.broadcasted_iota(jnp.int32, (tok, hd), 0)
    t_lane = lax.broadcasted_iota(jnp.int32, (tok, hd), 1)
    for o in range(CORES):
        hot = jnp.where(t_lane == t_row + o * tok, 1.0, 0.0).astype(jnp.bfloat16)
        for h in range(grp):
            qaug[o * grp + h, :, hd:2 * hd] = hot

    c_cu.wait()
    bounds = [cus[0, d] for d in range(n_docs + 1)]

    def coords(t):
        seg = jnp.full(t.shape, bounds[0], jnp.int32)
        loc = jnp.full(t.shape, lax.div(bounds[0], cp), jnp.int32)
        plen = jnp.full(t.shape, lax.div(bounds[1] - bounds[0], 2 * cp), jnp.int32)
        for d in range(1, n_docs):
            first = lax.div(bounds[d], cp)
            hit = t >= first
            seg = jnp.where(hit, bounds[d], seg)
            loc = jnp.where(hit, first, loc)
            plen = jnp.where(hit, lax.div(bounds[d + 1] - bounds[d], 2 * cp), plen)
        within = t - loc
        up = within >= plen
        base = seg + within + jnp.where(up, (2 * cp - 2) * plen, 0)
        return seg, base, jnp.where(up, -plen, plen)

    _, key_base, key_slope = coords(t_row)
    lane_q = lax.broadcasted_iota(jnp.int32, (8, keys), 1)
    seg_q, base_q, slope_q = coords(lax.rem(lane_q, tok))
    rank_q = jnp.where(lane_q < tok, me, partner)
    pos_q = base_q + rank_q * slope_q
    lo_b = jnp.broadcast_to(seg_q[0:1], (tok, keys))
    hi_b = jnp.broadcast_to(pos_q[0:1], (tok, keys))

    def prepare(blk):
        s = SLOT[blk]
        for o in range(CORES):
            rank = chip_at(*blk) * CORES + (core if o == 0 else 1 - core)
            pos = key_base + rank * key_slope
            kf = kv[0, s, o].astype(jnp.float32)
            invalid = jnp.broadcast_to(kf[:, 0:1], (tok, keys)) == jnp.inf
            seen = (pos >= lo_b) & (pos <= hi_b) & jnp.logical_not(invalid)
            kaug[s, o * tok:(o + 1) * tok, 0:hd] = jnp.where(kf == jnp.inf, 0.0, kf).astype(jnp.bfloat16)
            kaug[s, o * tok:(o + 1) * tok, hd:2 * hd] = jnp.where(seen, 0.0, NEG).astype(jnp.bfloat16)

    c2 = scale * math.log2(math.e)

    def scores(level):
        lo, n = SLOT[level[0]], len(level)
        for blk in level:
            prepare(blk)
        ka = kaug[lo:lo + n].reshape(n * keys, 2 * hd)
        sbuf[lo:lo + n] = dot(ka, qaug[...].reshape(rows, 2 * hd), NT).reshape(n, keys, rows)

    def grads_p(level):
        lo, n = SLOT[level[0]], len(level)
        vb = kv[1, lo:lo + n].reshape(n * keys, hd)
        dpbuf[lo:lo + n] = dot(vb, dob[...].reshape(rows, hd), NT).reshape(n, keys, rows)

    def softmax(level, first):
        lo, n = SLOT[level[0]], len(level)
        mx = jnp.max(sbuf[lo:lo + n].reshape(n * keys, rows), axis=0, keepdims=True)
        if first:
            m_new = mx
        else:
            m_old = m_ref[...]
            m_new = jnp.maximum(m_old, mx)
            alpha = jnp.exp2((m_old - m_new) * c2)
        m_ref[...] = m_new
        mc = m_new * c2
        total = None
        for i in range(n):
            p = jnp.exp2(sbuf[lo + i] * c2 - mc)
            pbuf[lo + i] = p.astype(jnp.bfloat16)
            part_sum = jnp.sum(p, axis=0, keepdims=True)
            total = part_sum if total is None else total + part_sum
        pv = dot(kv[1, lo:lo + n].reshape(n * keys, hd), pbuf[lo:lo + n].reshape(n * keys, rows), TN)
        if first:
            l_ref[...] = total
            o_t[...] = pv
        else:
            l_ref[...] = l_ref[...] * alpha + total
            o_t[...] = o_t[...] * alpha + pv

    for X in range(2):
        arrive(X, (0, 0), 1)
        forward(X, (0, 0), 1)
    c_q.wait()
    x_q.wait_recv()
    scores(LEVELS[0])
    c_do.wait()
    x_do.wait_recv()
    dot_t[...] = jnp.transpose(dob[...].reshape(rows, hd).astype(jnp.float32))
    softmax(LEVELS[0], True)
    grads_p(LEVELS[0])
    for level in LEVELS[1:]:
        for o in range(CORES):
            for blk in level:
                for X in range(2):
                    arrive(X, blk, o)
                    forward(X, blk, o)
        scores(level)
        softmax(level, False)
        grads_p(level)

    m_fin, l_fin = m_ref[...], l_ref[...]
    has_key = m_fin > NEG * 0.5
    safe = jnp.where(has_key, l_fin, 1.0)
    o_b = jnp.where(has_key, o_t[...] / safe, 0.0).astype(jnp.bfloat16).astype(jnp.float32)
    o_t[...] = o_b
    delta = jnp.sum(o_b * dot_t[...], axis=0, keepdims=True)
    lse = jnp.where(has_key, m_fin * scale + jnp.log(safe), 0.0)
    lse2 = jnp.where(has_key, m_fin * c2 + jnp.log2(safe), 0.0)

    rs_items = []

    def rsend(X, blk, o, key, step):
        i = RIDX[key]
        push(part.at[X, SLOT[blk], o], rbuf.at[X, i], rs_send.at[X, i], rs_recv.at[X, i], nbr(unframe(X, *step)))

    def rwait(X, key):
        i = RIDX[key]
        remote(rbuf.at[X, i], rbuf.at[X, i], rs_send.at[X, i], rs_recv.at[X, i], to_partner).wait_recv()
        return rbuf[X, i]

    def immediate(X, blk):
        a, b = frame(X, blk)
        if b == 2:
            rsend(X, blk, 0, ('rb', a, 0), (0, -1))
            rsend(X, blk, 1, ('rb', a, 1), (0, 1))
        elif b == 3:
            rsend(X, blk, 1, ('fb', a, 1, 1), (0, -1))
        elif b == 1:
            rsend(X, blk, 0, ('fb', a, 0, -1), (0, 1))

    def relay_b(X, a):
        for b, o, step, sgn in ((3, 0, -1, 1), (1, 1, 1, -1)):
            blk = unframe(X, a, b)
            part[X, SLOT[blk], o] += rwait(X, ('rb', a, o))
            rsend(X, blk, o, ('fb', a, o, sgn), (0, step))

    def gather_b(X, a, o):
        blk = unframe(X, a, 0)
        part[X, SLOT[blk], o] += rwait(X, ('fb', a, o, 1)) + rwait(X, ('fb', a, o, -1))
        return blk

    def relay_a(X, a, o):
        blk = gather_b(X, a, o)
        if a == 2:
            rsend(X, blk, o, ('ra', o), (-1 if o == 0 else 1, 0))
        else:
            if (a == 3) == (o == 0):
                part[X, SLOT[blk], o] += rwait(X, ('ra', o))
            rsend(X, blk, o, ('fa', o, 1 if a == 3 else -1), (-1 if a == 3 else 1, 0))

    dob2 = dob[...].reshape(rows, hd)

    def backward(blk):
        s = SLOT[blk]
        p = jnp.exp2(sbuf[s] * c2 - lse2)
        pbuf[s] = p.astype(jnp.bfloat16)
        dsbuf[s] = (p * (dpbuf[s] - delta)).astype(jnp.bfloat16)
        part[1, s] = dot(pbuf[s], dob[...].reshape(rows, hd)).reshape(CORES, tok, hd)
        part[0, s] = dot(dsbuf[s], qaug[:, :, 0:hd].reshape(rows, hd)).reshape(CORES, tok, hd)
        for X in range(2):
            immediate(X, blk)

    for level in (LEVELS[4], LEVELS[3], LEVELS[2]):
        for blk in level:
            backward(blk)
    for X in range(2):
        relay_b(X, 2)
    for blk in LEVELS[1]:
        backward(blk)
    for a in (1, 3, 0):
        for X in range(2):
            relay_b(X, a)
    backward((0, 0))
    for o in range(CORES):
        for X in range(2):
            relay_a(X, 2, o)

    o_rows = jnp.transpose(o_t[...]).astype(jnp.bfloat16).reshape(2 * grp, tok, hd)
    ost[...] = o_rows
    for o in range(CORES):
        for h in range(grp):
            j = (o * grp + h) * tok
            lsest[o, h:h + 1, :] = lse[:, j:j + tok]
    w_o = pltpu.make_async_copy(ost.at[0:grp], o_hbm.at[pl.ds(mine, grp)], loc_sem.at[0])
    w_l = pltpu.make_async_copy(lsest.at[0], lse_hbm.at[core], loc_sem.at[1])
    w_o.start()
    w_l.start()
    x_o = push(ost.at[grp:2 * grp], o_hbm.at[pl.ds(mine, grp)], pair_send.at[4], pair_recv.at[4], to_partner)
    x_l = push(lsest.at[1], lse_hbm.at[core], pair_send.at[5], pair_recv.at[5], to_partner)
    dq_t = dot(kaug[:, :, 0:hd].reshape(NBLK * keys, hd), dsbuf[...].reshape(NBLK * keys, rows), TN)
    dqst[...] = (jnp.transpose(dq_t) * scale).astype(jnp.bfloat16).reshape(2 * grp, tok, hd)
    w_q = pltpu.make_async_copy(dqst.at[0:grp], dq_hbm.at[pl.ds(mine, grp)], loc_sem.at[2])
    w_q.start()
    x_dq = push(dqst.at[grp:2 * grp], dq_hbm.at[pl.ds(mine, grp)], pair_send.at[6], pair_recv.at[6], to_partner)

    for a in (1, 3):
        for o in range(CORES):
            for X in range(2):
                relay_a(X, a, o)

    def final(X, o):
        gather_b(X, 0, o)
        total = part[X, 0, o] + rwait(X, ('fa', o, 1)) + rwait(X, ('fa', o, -1))
        if X == 0:
            total = total * scale
        return total.astype(jnp.bfloat16)

    x_kv = []
    for X in range(2):
        kvsend[X] = final(X, 1)
        x_kv.append(push(kvsend.at[X], kvrecv.at[X], pair_send.at[7 + X], pair_recv.at[7 + X], to_partner))
    owns = [final(X, 0).astype(jnp.float32) for X in range(2)]
    w_kv = []
    for X, out in ((0, dk_hbm), (1, dv_hbm)):
        x_kv[X].wait_recv()
        got = kvrecv[X].astype(jnp.float32)
        tmp32[X, pl.ds(0, tok, stride=2), :] = jnp.where(core == 0, owns[X], got)
        tmp32[X, pl.ds(1, tok, stride=2), :] = jnp.where(core == 0, got, owns[X])
        outb[X] = tmp32[X].astype(jnp.bfloat16)
        w = pltpu.make_async_copy(outb.at[X], out, loc_sem.at[3 + X])
        w.start()
        w_kv.append(w)
    for c in sends:
        c.wait_send()
    for x in (x_o, x_l, x_dq):
        x.wait_recv()
    for w in [w_o, w_l, w_q] + w_kv:
        w.wait()


def solution(mesh):
    cp = mesh.shape['cp']
    tok_spec = P(('dp', 'cp'), None, None)

    def local(q, k, v, do, valid, cu):
        tok, heads, hd = q.shape
        kvh = k.shape[1]
        grp = heads // kvh
        n_docs = cu.shape[0] - 1
        rows = CORES * grp * tok
        keys = CORES * tok
        assert kvh == CORES and cp == CORES * SIDE * SIDE and keys == hd
        bf, f32 = jnp.bfloat16, jnp.float32
        any_spec = pl.BlockSpec(memory_space=pl.ANY)
        n_rs = len(RKEYS)
        flat = lambda x: x.reshape(tok * kvh, hd)
        o, lse, dq, dk, dv = pl.pallas_call(
            functools.partial(kernel, cp, n_docs, hd ** -0.5),
            name='ring_attention',
            out_shape=[
                jax.ShapeDtypeStruct((heads, tok, hd), bf),
                jax.ShapeDtypeStruct((CORES, grp, tok), f32),
                jax.ShapeDtypeStruct((heads, tok, hd), bf),
                jax.ShapeDtypeStruct((tok * kvh, hd), bf),
                jax.ShapeDtypeStruct((tok * kvh, hd), bf),
            ],
            in_specs=[any_spec] * 6,
            out_specs=[any_spec] * 5,
            scratch_shapes=[
                pltpu.VMEM((2, tok * kvh, hd), bf),
                pltpu.VMEM((2, tok * kvh, hd), f32),
                pltpu.VMEM((2, tok, hd), bf),
                pltpu.VMEM((2, NBLK, CORES, tok, hd), bf),
                pltpu.VMEM((NBLK, keys, 2 * hd), bf),
                pltpu.VMEM((CORES * grp, tok, 2 * hd), bf),
                pltpu.VMEM((CORES * grp, tok, hd), bf),
                pltpu.VMEM((hd, rows), f32),
                pltpu.VMEM((NBLK, keys, rows), f32),
                pltpu.VMEM((NBLK, keys, rows), f32),
                pltpu.VMEM((NBLK, keys, rows), bf),
                pltpu.VMEM((NBLK, keys, rows), bf),
                pltpu.VMEM((2, NBLK, CORES, tok, hd), f32),
                pltpu.VMEM((2, n_rs, tok, hd), f32),
                pltpu.VMEM((CORES * grp, tok, hd), bf),
                pltpu.VMEM((CORES * grp, tok, hd), bf),
                pltpu.VMEM((CORES, grp, tok), f32),
                pltpu.VMEM((2, tok, hd), bf),
                pltpu.VMEM((2, tok, hd), bf),
                pltpu.VMEM((2, tok * kvh, hd), f32),
                pltpu.VMEM((2, tok * kvh, hd), bf),
                pltpu.VMEM((1, rows), f32),
                pltpu.VMEM((1, rows), f32),
                pltpu.VMEM((hd, rows), f32),
                pltpu.VMEM((1, tok), jnp.int32),
                pltpu.SMEM((1, n_docs + 1), jnp.int32),
                pltpu.SemaphoreType.DMA((6,)),
                pltpu.SemaphoreType.DMA((9,)),
                pltpu.SemaphoreType.DMA((9,)),
                pltpu.SemaphoreType.DMA((64,)),
                pltpu.SemaphoreType.DMA((2, NBLK, CORES)),
                pltpu.SemaphoreType.DMA((2, n_rs)),
                pltpu.SemaphoreType.DMA((2, n_rs)),
            ],
            compiler_params=pltpu.CompilerParams(
                collective_id=0, has_side_effects=True, vmem_limit_bytes=60 * 1024 * 1024),
        )(q.transpose(1, 0, 2), flat(k), flat(v), do.transpose(1, 0, 2), valid.reshape(1, tok), cu.reshape(1, n_docs + 1))
        back = lambda x: x.reshape(tok, kvh, hd)
        return (o.transpose(1, 0, 2), lse.reshape(heads, tok).transpose(1, 0), dq.transpose(1, 0, 2), back(dk), back(dv))

    return jax.shard_map(
        local, mesh=mesh,
        in_specs=(tok_spec, tok_spec, tok_spec, tok_spec, P(('dp', 'cp')), P('dp')),
        out_specs=(tok_spec, P(('dp', 'cp'), None), tok_spec, tok_spec, tok_spec), check_vma=False)
```

```python
import functools
import math

import jax
import jax.numpy as jnp
from jax import lax
from jax.experimental import pallas as pl
from jax.experimental.pallas import tpu as pltpu
from jax.sharding import PartitionSpec as P

MESH = pl.DeviceIdType.MESH
scope = jax.named_scope
NEG = -(2.0 ** 126)
CORES = 2
SIDE = 4
LEVELS = (
    ((0, 0),),
    ((1, 0), (3, 0), (0, 1), (0, 3)),
    ((2, 0), (0, 2), (1, 1), (1, 3), (3, 1), (3, 3)),
    ((2, 1), (2, 3), (1, 2), (3, 2)),
    ((2, 2),),
)
BLOCKS = tuple(blk for level in LEVELS for blk in level)
SLOT = {blk: i for i, blk in enumerate(BLOCKS)}
NBLK = len(BLOCKS)
NT = (((1,), (1,)), ((), ()))
TN = (((0,), (0,)), ((), ()))


def dot(a, b, dims=(((1,), (0,)), ((), ()))):
    return lax.dot_general(a, b, dims, preferred_element_type=jnp.float32)


def frame(X, blk):
    return blk if X == 0 else (blk[1], blk[0])


def unframe(X, a, b):
    return (a, b) if X == 0 else (b, a)


def routes(X, blk, o):
    a, b = frame(X, blk)
    out = []
    if b == 0:
        if a == 3 and o == 0:
            out.append((1, 0))
        if a == 1 and o == 1:
            out.append((-1, 0))
        if a == 0:
            out += [(1, 0), (-1, 0)]
        out += [(0, 1), (0, -1)]
    elif b == 3 and o == 0:
        out.append((0, 1))
    elif b == 1 and o == 1:
        out.append((0, -1))
    return [unframe(X, *step) for step in out]


RKEYS = []
for _a in range(SIDE):
    RKEYS += [('rb', _a, 0), ('rb', _a, 1)]
    RKEYS += [('fb', _a, _o, _s) for _o in range(2) for _s in (1, -1)]
RKEYS += [('ra', 0), ('ra', 1)]
RKEYS += [('fa', _o, _s) for _o in range(2) for _s in (1, -1)]
RIDX = {key: i for i, key in enumerate(RKEYS)}


def kernel(cp, n_docs, scale, q_hbm, k_hbm, v_hbm, do_hbm, val_hbm, cu_hbm,
           o_out, lse_out, dq_out, dk_out, dv_out,
           kin, kf32, oth, kv, kaug, qaug, dob, dot_t, sbuf, dpbuf, pbuf, dsbuf, part, rbuf,
           ost, dqst, lsest, kvsend, kvrecv, tmp32, m_ref, l_ref, o_t, valv, cus,
           loc_sem, pair_send, pair_recv, ag_send, ag_recv, rs_send, rs_recv):
    tok = valv.shape[1]
    grp = ost.shape[0]
    rows = CORES * grp * tok
    hd = kin.shape[-1]
    keys = CORES * tok
    me = lax.axis_index('cp')
    core = lax.rem(me, CORES)
    chip = lax.div(me, CORES)
    cx = lax.rem(chip, SIDE)
    cy = lax.div(chip, SIDE)
    partner = me + 1 - 2 * core

    def chip_at(dx, dy):
        return lax.rem(cy + dy + SIDE, SIDE) * SIDE + lax.rem(cx + dx + SIDE, SIDE)

    def nbr(step):
        return {'cp': chip_at(*step) * CORES + core}

    mine = core * grp
    theirs = (1 - core) * grp
    to_partner = {'cp': partner}

    c_k = pltpu.make_async_copy(k_hbm, kin.at[0], loc_sem.at[0])
    c_v = pltpu.make_async_copy(v_hbm, kin.at[1], loc_sem.at[1])
    c_val = pltpu.make_async_copy(val_hbm, valv, loc_sem.at[2])
    c_cu = pltpu.make_async_copy(cu_hbm, cus, loc_sem.at[3])
    c_q = pltpu.make_async_copy(q_hbm.at[pl.ds(mine, grp)], qaug.at[0:grp, :, 0:hd], loc_sem.at[4])
    c_do = pltpu.make_async_copy(do_hbm.at[pl.ds(mine, grp)], dob.at[0:grp], loc_sem.at[5])
    for c in (c_k, c_v, c_val, c_cu, c_q, c_do):
        c.start()

    barrier = pltpu.get_barrier_semaphore()
    peers = [to_partner] + [nbr(s) for s in ((1, 0), (-1, 0), (0, 1), (0, -1))]
    for peer in peers:
        pl.semaphore_signal(barrier, inc=1, device_id=peer, device_id_type=MESH)

    sends = []

    def remote(src, dst, ssem, rsem, dev):
        copy = pltpu.make_async_remote_copy(src_ref=src, dst_ref=dst, send_sem=ssem, recv_sem=rsem,
                                            device_id=dev, device_id_type=MESH)
        return copy

    def push(src, dst, ssem, rsem, dev):
        copy = remote(src, dst, ssem, rsem, dev)
        copy.start()
        sends.append(copy)
        return copy

    with scope('load_kv'):
        for c in (c_k, c_v, c_val):
            c.wait()
    sub = lax.broadcasted_iota(jnp.int32, (tok, tok), 0)
    lane = lax.broadcasted_iota(jnp.int32, (tok, tok), 1)
    vcol = jnp.sum(jnp.where(sub == lane, jnp.broadcast_to(valv[...], (tok, tok)), 0), axis=1, keepdims=True)
    lane0 = lax.broadcasted_iota(jnp.int32, (tok, hd), 1) == 0
    bad = lane0 & (jnp.broadcast_to(vcol, (tok, hd)) <= 0)
    for X in range(2):
        kf32[X] = kin[X].astype(jnp.float32)
    for X in range(2):
        h0 = kf32[X, pl.ds(0, tok, stride=2), :]
        h1 = kf32[X, pl.ds(1, tok, stride=2), :]
        own = jnp.where(core == 0, h0, h1)
        other = jnp.where(core == 0, h1, h0)
        if X == 0:
            own = jnp.where(bad, jnp.inf, own)
            other = jnp.where(bad, jnp.inf, other)
        kv[X, 0, 0] = own.astype(jnp.bfloat16)
        oth[X] = other.astype(jnp.bfloat16)

    with scope('barrier'):
        pl.semaphore_wait(barrier, len(peers))

    ag_count = [0]

    def forward(X, blk, o):
        for step in routes(X, blk, o):
            dst_blk = ((blk[0] - step[0]) % SIDE, (blk[1] - step[1]) % SIDE)
            s = SLOT[dst_blk]
            push(kv.at[X, SLOT[blk], o], kv.at[X, s, o], ag_send.at[ag_count[0]], ag_recv.at[X, s, o], nbr(step))
            ag_count[0] += 1

    def arrive(X, blk, o):
        s = SLOT[blk]
        remote(kv.at[X, s, o], kv.at[X, s, o], ag_send.at[0], ag_recv.at[X, s, o], to_partner).wait_recv()

    for X in range(2):
        push(oth.at[X], kv.at[X, 0, 1], pair_send.at[X], ag_recv.at[X, 0, 1], to_partner)
    for X in range(2):
        forward(X, (0, 0), 0)
    x_q = push(q_hbm.at[pl.ds(theirs, grp)], qaug.at[grp:2 * grp, :, 0:hd], pair_send.at[2], pair_recv.at[2], to_partner)
    x_do = push(do_hbm.at[pl.ds(theirs, grp)], dob.at[grp:2 * grp], pair_send.at[3], pair_recv.at[3], to_partner)

    t_row = lax.broadcasted_iota(jnp.int32, (tok, hd), 0)
    t_lane = lax.broadcasted_iota(jnp.int32, (tok, hd), 1)
    for o in range(CORES):
        hot = jnp.where(t_lane == t_row + o * tok, 1.0, 0.0).astype(jnp.bfloat16)
        for h in range(grp):
            qaug[o * grp + h, :, hd:2 * hd] = hot

    with scope('wait_cu'):
        c_cu.wait()
    bounds = [cus[0, d] for d in range(n_docs + 1)]

    def coords(t):
        seg = jnp.full(t.shape, bounds[0], jnp.int32)
        loc = jnp.full(t.shape, lax.div(bounds[0], cp), jnp.int32)
        plen = jnp.full(t.shape, lax.div(bounds[1] - bounds[0], 2 * cp), jnp.int32)
        for d in range(1, n_docs):
            first = lax.div(bounds[d], cp)
            hit = t >= first
            seg = jnp.where(hit, bounds[d], seg)
            loc = jnp.where(hit, first, loc)
            plen = jnp.where(hit, lax.div(bounds[d + 1] - bounds[d], 2 * cp), plen)
        within = t - loc
        up = within >= plen
        base = seg + within + jnp.where(up, (2 * cp - 2) * plen, 0)
        return seg, base, jnp.where(up, -plen, plen)

    _, key_base, key_slope = coords(t_row)
    lane_q = lax.broadcasted_iota(jnp.int32, (8, keys), 1)
    seg_q, base_q, slope_q = coords(lax.rem(lane_q, tok))
    rank_q = jnp.where(lane_q < tok, me, partner)
    pos_q = base_q + rank_q * slope_q
    lo_b = jnp.broadcast_to(seg_q[0:1], (tok, keys))
    hi_b = jnp.broadcast_to(pos_q[0:1], (tok, keys))

    def prepare(blk):
        s = SLOT[blk]
        for o in range(CORES):
            rank = chip_at(*blk) * CORES + (core if o == 0 else 1 - core)
            pos = key_base + rank * key_slope
            kf = kv[0, s, o].astype(jnp.float32)
            invalid = jnp.broadcast_to(kf[:, 0:1], (tok, keys)) == jnp.inf
            seen = (pos >= lo_b) & (pos <= hi_b) & jnp.logical_not(invalid)
            kaug[s, o * tok:(o + 1) * tok, 0:hd] = jnp.where(kf == jnp.inf, 0.0, kf).astype(jnp.bfloat16)
            kaug[s, o * tok:(o + 1) * tok, hd:2 * hd] = jnp.where(seen, 0.0, NEG).astype(jnp.bfloat16)

    c2 = scale * math.log2(math.e)

    def scores(level):
        lo, n = SLOT[level[0]], len(level)
        for blk in level:
            prepare(blk)
        ka = kaug[lo:lo + n].reshape(n * keys, 2 * hd)
        sbuf[lo:lo + n] = dot(ka, qaug[...].reshape(rows, 2 * hd), NT).reshape(n, keys, rows)

    def grads_p(level):
        lo, n = SLOT[level[0]], len(level)
        vb = kv[1, lo:lo + n].reshape(n * keys, hd)
        dpbuf[lo:lo + n] = dot(vb, dob[...].reshape(rows, hd), NT).reshape(n, keys, rows)

    def softmax(level, first):
        lo, n = SLOT[level[0]], len(level)
        mx = jnp.max(sbuf[lo:lo + n].reshape(n * keys, rows), axis=0, keepdims=True)
        if first:
            m_new = mx
        else:
            m_old = m_ref[...]
            m_new = jnp.maximum(m_old, mx)
            alpha = jnp.exp2((m_old - m_new) * c2)
        m_ref[...] = m_new
        mc = m_new * c2
        total = None
        for i in range(n):
            p = jnp.exp2(sbuf[lo + i] * c2 - mc)
            pbuf[lo + i] = p.astype(jnp.bfloat16)
            part_sum = jnp.sum(p, axis=0, keepdims=True)
            total = part_sum if total is None else total + part_sum
        pv = dot(kv[1, lo:lo + n].reshape(n * keys, hd), pbuf[lo:lo + n].reshape(n * keys, rows), TN)
        if first:
            l_ref[...] = total
            o_t[...] = pv
        else:
            l_ref[...] = l_ref[...] * alpha + total
            o_t[...] = o_t[...] * alpha + pv

    with scope('pair_kv'):
        for X in range(2):
            arrive(X, (0, 0), 1)
            forward(X, (0, 0), 1)
    with scope('pair_q'):
        c_q.wait()
        x_q.wait_recv()
    with scope('scores0'):
        scores(LEVELS[0])
    with scope('pair_do'):
        c_do.wait()
        x_do.wait_recv()
    with scope('do_t'):
        dot_t[...] = jnp.transpose(dob[...].reshape(rows, hd).astype(jnp.float32))
    with scope('softmax0'):
        softmax(LEVELS[0], True)
    with scope('grads_p0'):
        grads_p(LEVELS[0])
    for i, level in enumerate(LEVELS[1:], 1):
        with scope('gather%d' % i):
            for o in range(CORES):
                for blk in level:
                    for X in range(2):
                        arrive(X, blk, o)
                        forward(X, blk, o)
        with scope('scores%d' % i):
            scores(level)
        with scope('softmax%d' % i):
            softmax(level, False)
        with scope('grads_p%d' % i):
            grads_p(level)

    scope_fin = scope('finish')
    scope_fin.__enter__()
    m_fin, l_fin = m_ref[...], l_ref[...]
    has_key = m_fin > NEG * 0.5
    safe = jnp.where(has_key, l_fin, 1.0)
    o_b = jnp.where(has_key, o_t[...] / safe, 0.0).astype(jnp.bfloat16).astype(jnp.float32)
    o_t[...] = o_b
    delta = jnp.sum(o_b * dot_t[...], axis=0, keepdims=True)
    lse = jnp.where(has_key, m_fin * scale + jnp.log(safe), 0.0)
    lse2 = jnp.where(has_key, m_fin * c2 + jnp.log2(safe), 0.0)

    scope_fin.__exit__(None, None, None)

    def rsend(X, blk, o, key, step):
        i = RIDX[key]
        push(part.at[X, SLOT[blk], o], rbuf.at[X, i], rs_send.at[X, i], rs_recv.at[X, i], nbr(unframe(X, *step)))

    def rwait(X, key):
        i = RIDX[key]
        remote(rbuf.at[X, i], rbuf.at[X, i], rs_send.at[X, i], rs_recv.at[X, i], to_partner).wait_recv()
        return rbuf[X, i]

    def immediate(X, blk):
        a, b = frame(X, blk)
        if b == 2:
            rsend(X, blk, 0, ('rb', a, 0), (0, -1))
            rsend(X, blk, 1, ('rb', a, 1), (0, 1))
        elif b == 3:
            rsend(X, blk, 1, ('fb', a, 1, 1), (0, -1))
        elif b == 1:
            rsend(X, blk, 0, ('fb', a, 0, -1), (0, 1))

    def relay_b(X, a):
        for b, o, step, sgn in ((3, 0, -1, 1), (1, 1, 1, -1)):
            blk = unframe(X, a, b)
            part[X, SLOT[blk], o] += rwait(X, ('rb', a, o))
            rsend(X, blk, o, ('fb', a, o, sgn), (0, step))

    def gather_b(X, a, o):
        blk = unframe(X, a, 0)
        part[X, SLOT[blk], o] += rwait(X, ('fb', a, o, 1)) + rwait(X, ('fb', a, o, -1))
        return blk

    def relay_a(X, a, o):
        blk = gather_b(X, a, o)
        if a == 2:
            rsend(X, blk, o, ('ra', o), (-1 if o == 0 else 1, 0))
        else:
            if (a == 3) == (o == 0):
                part[X, SLOT[blk], o] += rwait(X, ('ra', o))
            rsend(X, blk, o, ('fa', o, 1 if a == 3 else -1), (-1 if a == 3 else 1, 0))

    def backward(blk):
        s = SLOT[blk]
        p = jnp.exp2(sbuf[s] * c2 - lse2)
        pbuf[s] = p.astype(jnp.bfloat16)
        dsbuf[s] = (p * (dpbuf[s] - delta)).astype(jnp.bfloat16)
        part[1, s] = dot(pbuf[s], dob[...].reshape(rows, hd)).reshape(CORES, tok, hd)
        part[0, s] = dot(dsbuf[s], qaug[:, :, 0:hd].reshape(rows, hd)).reshape(CORES, tok, hd)
        for X in range(2):
            immediate(X, blk)

    for level in (LEVELS[4], LEVELS[3], LEVELS[2]):
        for blk in level:
            with scope('bwd%d%d' % blk):
                backward(blk)
    with scope('relay_b2'):
        for X in range(2):
            relay_b(X, 2)
    for blk in LEVELS[1]:
        with scope('bwd%d%d' % blk):
            backward(blk)
    for a in (1, 3, 0):
        with scope('relay_b%d' % a):
            for X in range(2):
                relay_b(X, a)
    with scope('bwd00'):
        backward((0, 0))
    with scope('relay_a2'):
        for o in range(CORES):
            for X in range(2):
                relay_a(X, 2, o)

    scope_out = scope('out_o')
    scope_out.__enter__()
    o_rows = jnp.transpose(o_t[...]).astype(jnp.bfloat16).reshape(2 * grp, tok, hd)
    o_out[pl.ds(mine, grp)] = o_rows[0:grp]
    ost[...] = o_rows[grp:2 * grp]
    for h in range(grp):
        lse_out[core, h:h + 1, :] = lse[:, h * tok:(h + 1) * tok]
        lsest[h:h + 1, :] = lse[:, (grp + h) * tok:(grp + h + 1) * tok]
    x_o = push(ost, o_out.at[pl.ds(mine, grp)], pair_send.at[4], pair_recv.at[4], to_partner)
    x_l = push(lsest, lse_out.at[core], pair_send.at[5], pair_recv.at[5], to_partner)
    scope_out.__exit__(None, None, None)
    scope_out = scope('out_dq')
    scope_out.__enter__()
    dq_t = dot(kaug[:, :, 0:hd].reshape(NBLK * keys, hd), dsbuf[...].reshape(NBLK * keys, rows), TN)
    dq_rows = (jnp.transpose(dq_t) * scale).astype(jnp.bfloat16).reshape(2 * grp, tok, hd)
    dq_out[pl.ds(mine, grp)] = dq_rows[0:grp]
    dqst[...] = dq_rows[grp:2 * grp]
    x_dq = push(dqst, dq_out.at[pl.ds(mine, grp)], pair_send.at[6], pair_recv.at[6], to_partner)

    scope_out.__exit__(None, None, None)
    for a in (1, 3):
        with scope('relay_a%d' % a):
            for o in range(CORES):
                for X in range(2):
                    relay_a(X, a, o)

    def final(X, o):
        gather_b(X, 0, o)
        total = part[X, 0, o] + rwait(X, ('fa', o, 1)) + rwait(X, ('fa', o, -1))
        if X == 0:
            total = total * scale
        return total.astype(jnp.bfloat16)

    x_kv = []
    with scope('final1'):
        for X in range(2):
            kvsend[X] = final(X, 1)
            x_kv.append(push(kvsend.at[X], kvrecv.at[X], pair_send.at[7 + X], pair_recv.at[7 + X], to_partner))
    with scope('final0'):
        owns = [final(X, 0).astype(jnp.float32) for X in range(2)]
    scope_out = scope('tail')
    scope_out.__enter__()
    for X, out in ((0, dk_out), (1, dv_out)):
        x_kv[X].wait_recv()
        got = kvrecv[X].astype(jnp.float32)
        tmp32[X, pl.ds(0, tok, stride=2), :] = jnp.where(core == 0, owns[X], got)
        tmp32[X, pl.ds(1, tok, stride=2), :] = jnp.where(core == 0, got, owns[X])
        out[...] = tmp32[X].astype(jnp.bfloat16)
    for c in sends:
        c.wait_send()
    for x in (x_o, x_l, x_dq):
        x.wait_recv()
    scope_out.__exit__(None, None, None)


def store_kernel(o_in, lse_in, dq_in, dk_in, dv_in, o_out, lse_out, dq_out, dk_out, dv_out, lse_v, sem):
    copies = [pltpu.make_async_copy(a, b, sem.at[i]) for i, (a, b) in enumerate(
        ((o_in, o_out), (dq_in, dq_out), (dk_in, dk_out), (dv_in, dv_out), (lse_v, lse_out)))]
    for c in copies[:4]:
        c.start()
    grp = lse_in.shape[1]
    for i in range(lse_in.shape[0]):
        lse_v[i * grp:(i + 1) * grp, :] = lse_in[i]
    copies[4].start()
    for c in copies:
        c.wait()


def solution(mesh):
    cp = mesh.shape['cp']
    tok_spec = P(('dp', 'cp'), None, None)

    def local(q, k, v, do, valid, cu):
        tok, heads, hd = q.shape
        kvh = k.shape[1]
        grp = heads // kvh
        n_docs = cu.shape[0] - 1
        rows = CORES * grp * tok
        keys = CORES * tok
        assert kvh == CORES and cp == CORES * SIDE * SIDE and keys == hd
        bf, f32 = jnp.bfloat16, jnp.float32
        hbm_spec = pl.BlockSpec(memory_space=pltpu.HBM)
        vmem_spec = pl.BlockSpec(memory_space=pltpu.VMEM)
        n_rs = len(RKEYS)
        flat = lambda x: x.reshape(tok * kvh, hd)
        o, lse, dq, dk, dv = pl.pallas_call(
            functools.partial(kernel, cp, n_docs, hd ** -0.5),
            name='ring_attention',
            out_shape=[
                jax.ShapeDtypeStruct((heads, tok, hd), bf),
                jax.ShapeDtypeStruct((CORES, grp, tok), f32),
                jax.ShapeDtypeStruct((heads, tok, hd), bf),
                jax.ShapeDtypeStruct((tok * kvh, hd), bf),
                jax.ShapeDtypeStruct((tok * kvh, hd), bf),
            ],
            in_specs=[hbm_spec] * 6,
            out_specs=[vmem_spec] * 5,
            scratch_shapes=[
                pltpu.VMEM((2, tok * kvh, hd), bf),
                pltpu.VMEM((2, tok * kvh, hd), f32),
                pltpu.VMEM((2, tok, hd), bf),
                pltpu.VMEM((2, NBLK, CORES, tok, hd), bf),
                pltpu.VMEM((NBLK, keys, 2 * hd), bf),
                pltpu.VMEM((CORES * grp, tok, 2 * hd), bf),
                pltpu.VMEM((CORES * grp, tok, hd), bf),
                pltpu.VMEM((hd, rows), f32),
                pltpu.VMEM((NBLK, keys, rows), f32),
                pltpu.VMEM((NBLK, keys, rows), f32),
                pltpu.VMEM((NBLK, keys, rows), bf),
                pltpu.VMEM((NBLK, keys, rows), bf),
                pltpu.VMEM((2, NBLK, CORES, tok, hd), f32),
                pltpu.VMEM((2, n_rs, tok, hd), f32),
                pltpu.VMEM((grp, tok, hd), bf),
                pltpu.VMEM((grp, tok, hd), bf),
                pltpu.VMEM((grp, tok), f32),
                pltpu.VMEM((2, tok, hd), bf),
                pltpu.VMEM((2, tok, hd), bf),
                pltpu.VMEM((2, tok * kvh, hd), f32),
                pltpu.VMEM((1, rows), f32),
                pltpu.VMEM((1, rows), f32),
                pltpu.VMEM((hd, rows), f32),
                pltpu.VMEM((1, tok), jnp.int32),
                pltpu.SMEM((1, n_docs + 1), jnp.int32),
                pltpu.SemaphoreType.DMA((6,)),
                pltpu.SemaphoreType.DMA((9,)),
                pltpu.SemaphoreType.DMA((9,)),
                pltpu.SemaphoreType.DMA((64,)),
                pltpu.SemaphoreType.DMA((2, NBLK, CORES)),
                pltpu.SemaphoreType.DMA((2, n_rs)),
                pltpu.SemaphoreType.DMA((2, n_rs)),
            ],
            compiler_params=pltpu.CompilerParams(
                collective_id=0, has_side_effects=True, vmem_limit_bytes=40 * 1024 * 1024),
        )(*(pltpu.with_memory_space_constraint(a, pltpu.HBM) for a in (q.transpose(1, 0, 2), flat(k), flat(v), do.transpose(1, 0, 2), valid.reshape(1, tok), cu.reshape(1, n_docs + 1))))
        o, lse, dq, dk, dv = pl.pallas_call(
            store_kernel,
            name='store_outputs',
            out_shape=[
                jax.ShapeDtypeStruct((heads, tok, hd), bf),
                jax.ShapeDtypeStruct((heads, tok), f32),
                jax.ShapeDtypeStruct((heads, tok, hd), bf),
                jax.ShapeDtypeStruct((tok * kvh, hd), bf),
                jax.ShapeDtypeStruct((tok * kvh, hd), bf),
            ],
            in_specs=[vmem_spec] * 5,
            out_specs=[hbm_spec] * 5,
            scratch_shapes=[pltpu.VMEM((heads, tok), f32), pltpu.SemaphoreType.DMA((5,))],
            compiler_params=pltpu.CompilerParams(vmem_limit_bytes=1024 * 1024),
        )(o, lse, dq, dk, dv)
        back = lambda x: x.reshape(tok, kvh, hd)
        return (o.transpose(1, 0, 2), lse.transpose(1, 0), dq.transpose(1, 0, 2), back(dk), back(dv))

    return jax.shard_map(
        local, mesh=mesh,
        in_specs=(tok_spec, tok_spec, tok_spec, tok_spec, P(('dp', 'cp')), P('dp')),
        out_specs=(tok_spec, P(('dp', 'cp'), None), tok_spec, tok_spec, tok_spec), check_vma=False)
```

```python
import functools
import math

import jax
import jax.numpy as jnp
from jax import lax
from jax.experimental import pallas as pl
from jax.experimental.pallas import tpu as pltpu
from jax.sharding import PartitionSpec as P

MESH = pl.DeviceIdType.MESH
scope = jax.named_scope
NEG = -(2.0 ** 126)
CORES = 2
SIDE = 4
GROUPS = (
    ((0, 0),),
    ((1, 0), (3, 0), (0, 1), (0, 3)),
    ((1, 1), (1, 3), (3, 1), (3, 3)),
    ((2, 0), (0, 2)),
    ((2, 1), (2, 3), (1, 2), (3, 2)),
    ((2, 2),),
)
BLOCKS = tuple(blk for group in GROUPS for blk in group)
SLOT = {blk: i for i, blk in enumerate(BLOCKS)}
NBLK = len(BLOCKS)
GATHER = (
    (0, 0, 0, 0, 0, 2), (0, 0, 0, 0, 0, 1), (1, 0, 0, 0, 0, 1), (1, 0, 0, 0, 0, 2), (1, 0, 0, 0, 0, -1),
    (0, 0, 0, 0, 0, -1), (0, 0, 0, 1, 0, -1), (0, 0, 0, 1, 0, 2), (1, 0, 0, 1, 1, 2), (1, 0, 0, 1, 0, 2),
    (0, 0, 0, 0, 1, 2), (0, 0, 0, 1, 0, 1), (1, 0, 0, 1, 0, -1), (1, 0, 0, 0, 1, 2), (0, 0, 0, 1, 1, 1),
    (1, 0, 0, 1, 1, 1), (1, 0, 0, 0, 1, -1), (1, 0, 0, 1, 1, -1), (1, 0, 0, 0, 1, 1), (1, 0, 0, 1, 0, 1),
    (0, 0, 0, 1, 1, -1), (0, 0, 0, 0, 1, -1), (0, 0, 0, 0, 1, 1), (0, 1, 0, 0, 1, 2), (1, 1, 0, 0, 1, 2),
    (0, 2, 0, 0, 1, -1), (0, 0, 0, 1, 1, 2), (1, 2, 0, 0, 1, 2), (0, 2, 0, 0, 1, 2), (1, 2, 0, 0, 1, 1),
    (0, 2), (1, 2, 0, 0, 1, -1), (0, 1, 0, 0, 1, -1), (0, 3, 0, 0, 1, 2), (1, 1, 0, 1, 1, 2),
    (0, 1, 0, 1, 1, 2), (1, 2, 0, 1, 1, 2), (0, 2, 0, 1, 1, 2), (1, 2, 0, 1, 1, 1), (0, 0),
    (1, 2, 0, 1, 1, -1), (3, 2), (0, 3, 0, 1, 1, 2), (1, 3, 0, 1, 1, 2), (1, 3, 0, 0, 1, 2),
    (0, 2, 0, 0, 1, 1), (0, 2, 0, 1, 1, -1), (1, 2), (1, 3, 0, 1, 1, 1), (0, 2, 0, 1, 1, 1),
    (1, 0), (0, 1, 0, 1, 1, -1), (0, 1), (1, 3, 0, 1, 1, -1), (1, 3, 0, 0, 1, 1),
    (0, 1, 0, 0, 1, 1), (0, 3, 0, 1, 1, -1), (1, 3, 0, 0, 1, -1), (1, 1, 0, 1, 1, -1), (1, 1),
    (0, 3, 0, 0, 1, 1), (0, 3, 0, 1, 1, 1), (0, 1, 0, 1, 1, 1), (0, 3, 0, 0, 1, -1), (1, 1, 0, 0, 1, -1),
    (1, 1, 0, 1, 1, 1), (1, 1, 0, 0, 1, 1), (3, 0), (3, 1), (5, 2),
    (5, 0), (5, 1), (4, 2), (4, 0), (4, 1),
    (2, 0), (2, 1),
)
SCATTER = (
    (2, 1), (0, 2, 1, 0), (1, 1, 2, 0), (2, 2), (0, 2, 2, 0), (1, 2, 2, 1), (0, 2, 2, 1), (3, 2),
    (0, 3, 2, 1), (0, 3, 2, 0), (1, 1, 2, 1), (1, 2, 3, 1), (1, 2), (0, 2), (1, 2, 2, 0), (0, 1, 2, 0),
    (2, 3), (2, 0), (1, 3, 2, 1), (0, 0, 2, 1), (0, 0, 2, 0), (1, 0, 2, 0), (0, 1, 2, 1), (1, 0, 2, 1),
    (2, 2, -1), (1, 3), (1, 3, 2, 0), (0, 0), (0, 1, 3, 1), (1, 3, 1, 0), (3, 3), (1, 1),
    (0, 3, 3, 1), (3, 1), (0, 3, 1, 0), (1, 1, 1, 0), (1, 3, 3, 1), (1, 1, 3, 1), (0, 2, 3, 1), (0, 2, 3, 0),
    (1, 1, 1, 1), (0, 2, 1, 1), (0, 3, 1, 1), (0, 1), (3, 0), (0, 3), (1, 2, 3, 0), (0, 1, 3, 0),
    (1, 2, 1, 1), (1, 3, 1, 1), (1, 1, 3, 0), (0, 0, 3, 0), (0, 1, 1, 1), (1, 0), (0, 0, 1, 1), (0, 1, 1, 0),
    (1, 2, 1, 0), (1, 0, 3, 1), (1, 3, 3, 0), (0, 3, 3, 0), (1, 0, 1, 1), (0, 3, 0, 1), (1,), (1, 1, 0, 1),
    (0, 2, 0, 1), (1, 2, 0, 1), (0, 0, 1, 0), (0, 2, 0, 0), (0, 0, 3, 1), (1, 0, 3, 0), (0, 1, 0, 1), (1, 0, 1, 0),
    (1, 3, 0, 1), (0, 1, 0, 0), (1, 2, 0, 0), (1, 1, 0, 0), (1, 3, 0, 0), (0,), (0, 3, 0, 0), (0, 0, 0, 1),
    (1, 0, 0, 1), (1, 0, 0, 0), (0, 0, 0, 0),
)
NT = (((1,), (1,)), ((), ()))
TN = (((0,), (0,)), ((), ()))


def dot(a, b, dims=(((1,), (0,)), ((), ()))):
    return lax.dot_general(a, b, dims, preferred_element_type=jnp.float32)


def frame(X, blk):
    return blk if X == 0 else (blk[1], blk[0])


def unframe(X, a, b):
    return (a, b) if X == 0 else (b, a)


def terms(a, b, o):
    if b == 3:
        return [('rb', a, o)] if o == 0 else []
    if b == 1:
        return [('rb', a, o)] if o == 1 else []
    if b == 2:
        return []
    out = [('fb', a, o, 1), ('fb', a, o, -1)]
    if a == 0:
        out += [('fa', o, 1), ('fa', o, -1), ('ra', o)]
    return out


def target(a, b, o):
    if b == 2:
        return (0, -1 if o == 0 else 1), ('rb', a, o)
    if b:
        return (0, -1 if b == 3 else 1), ('fb', a, o, 1 if b == 3 else -1)
    if a == 2:
        return (2, 0), ('ra', o)
    return (-1 if a == 3 else 1, 0), ('fa', o, 1 if a == 3 else -1)


RIDX = {}
for _a in range(SIDE):
    for _b in range(SIDE):
        for _o in range(CORES):
            if (_a, _b) != (0, 0):
                RIDX[target(_a, _b, _o)[1]] = len(RIDX)


def kernel(cp, n_docs, scale, q_hbm, k_hbm, v_hbm, do_hbm, val_hbm, cu_hbm,
           o_out, lse_out, dq_out, dk_out, dv_out,
           kin, kf32, oth, kv, kaug, qbuf, qt, dob, dot_t, dot_b, sbuf, dpbuf, pbuf, dsbuf, part, rbuf,
           ost, dqst, lsest, kvsend, kvrecv, tmp32, m_ref, l_ref, o_t, valv, cus,
           loc_sem, pair_send, pair_recv, ag_send, ag_recv, rs_send, rs_recv):
    tok = valv.shape[1]
    grp = ost.shape[0]
    rows = CORES * grp * tok
    hd = kin.shape[-1]
    keys = CORES * tok
    me = lax.axis_index('cp')
    core = lax.rem(me, CORES)
    chip = lax.div(me, CORES)
    cx = lax.rem(chip, SIDE)
    cy = lax.div(chip, SIDE)
    partner = me + 1 - 2 * core

    def chip_at(dx, dy):
        return lax.rem(cy + dy + SIDE, SIDE) * SIDE + lax.rem(cx + dx + SIDE, SIDE)

    def nbr(step):
        return {'cp': chip_at(*step) * CORES + core}

    mine = core * grp
    theirs = (1 - core) * grp
    to_partner = {'cp': partner}

    c_k = pltpu.make_async_copy(k_hbm, kin.at[0], loc_sem.at[0])
    c_v = pltpu.make_async_copy(v_hbm, kin.at[1], loc_sem.at[1])
    c_val = pltpu.make_async_copy(val_hbm, valv, loc_sem.at[2])
    c_cu = pltpu.make_async_copy(cu_hbm, cus, loc_sem.at[3])
    c_q = pltpu.make_async_copy(q_hbm.at[pl.ds(mine, grp)], qbuf.at[0:grp], loc_sem.at[4])
    c_do = pltpu.make_async_copy(do_hbm.at[pl.ds(mine, grp)], dob.at[0:grp], loc_sem.at[5])
    for c in (c_k, c_v, c_val, c_cu, c_q, c_do):
        c.start()

    barrier = pltpu.get_barrier_semaphore()
    peers = [to_partner] + [nbr(s) for s in ((1, 0), (-1, 0), (2, 0), (0, 1), (0, -1), (0, 2))]
    for peer in peers:
        pl.semaphore_signal(barrier, inc=1, device_id=peer, device_id_type=MESH)

    sends = []

    def remote(src, dst, ssem, rsem, dev):
        copy = pltpu.make_async_remote_copy(src_ref=src, dst_ref=dst, send_sem=ssem, recv_sem=rsem,
                                            device_id=dev, device_id_type=MESH)
        return copy

    def push(src, dst, ssem, rsem, dev):
        copy = remote(src, dst, ssem, rsem, dev)
        copy.start()
        sends.append(copy)
        return copy

    with scope('load_kv'):
        for c in (c_k, c_v, c_val):
            c.wait()
    sub = lax.broadcasted_iota(jnp.int32, (tok, tok), 0)
    lane = lax.broadcasted_iota(jnp.int32, (tok, tok), 1)
    vcol = jnp.sum(jnp.where(sub == lane, jnp.broadcast_to(valv[...], (tok, tok)), 0), axis=1, keepdims=True)
    lane0 = lax.broadcasted_iota(jnp.int32, (tok, hd), 1) == 0
    bad = lane0 & (jnp.broadcast_to(vcol, (tok, hd)) <= 0)
    for X in range(2):
        kf32[X] = kin[X].astype(jnp.float32)
    for X in range(2):
        h0 = kf32[X, pl.ds(0, tok, stride=2), :]
        h1 = kf32[X, pl.ds(1, tok, stride=2), :]
        own = jnp.where(core == 0, h0, h1)
        other = jnp.where(core == 0, h1, h0)
        if X == 0:
            own = jnp.where(bad, jnp.inf, own)
            other = jnp.where(bad, jnp.inf, other)
        kv[X, 0, 0] = own.astype(jnp.bfloat16)
        oth[X] = other.astype(jnp.bfloat16)

    with scope('barrier'):
        pl.semaphore_wait(barrier, len(peers))

    here = {(X, (0, 0), 0) for X in range(2)}
    ag_count = [0]

    def arrive(X, blk, o):
        if (X, blk, o) not in here:
            s = SLOT[blk]
            remote(kv.at[X, s, o], kv.at[X, s, o], ag_send.at[0], ag_recv.at[X, s, o], to_partner).wait_recv()
            here.add((X, blk, o))

    def forward(X, a, b, o, phase, step):
        blk = unframe(X, a, b)
        arrive(X, blk, o)
        step = unframe(X, step * (1 - phase), step * phase)
        d = SLOT[(blk[0] - step[0]) % SIDE, (blk[1] - step[1]) % SIDE]
        push(kv.at[X, SLOT[blk], o], kv.at[X, d, o], ag_send.at[ag_count[0]], ag_recv.at[X, d, o], nbr(step))
        ag_count[0] += 1

    for X in range(2):
        push(oth.at[X], kv.at[X, 0, 1], pair_send.at[X], ag_recv.at[X, 0, 1], to_partner)
    early = 0
    while len(GATHER[early]) == 6 and GATHER[early][1:4] == (0, 0, 0):
        forward(*GATHER[early])
        early += 1
    x_q = push(q_hbm.at[pl.ds(theirs, grp)], qbuf.at[grp:2 * grp], pair_send.at[2], pair_recv.at[2], to_partner)
    x_do = push(do_hbm.at[pl.ds(theirs, grp)], dob.at[grp:2 * grp], pair_send.at[3], pair_recv.at[3], to_partner)

    t_row = lax.broadcasted_iota(jnp.int32, (tok, hd), 0)
    t_sub = lax.broadcasted_iota(jnp.int32, (keys, rows), 0)
    t_lane = lax.broadcasted_iota(jnp.int32, (keys, rows), 1)
    token = lax.rem(t_lane, tok) + jnp.where(t_lane >= grp * tok, tok, 0)
    qt[hd:hd + keys, :] = jnp.where(t_sub == token, 1.0, 0.0).astype(jnp.bfloat16)

    with scope('wait_cu'):
        c_cu.wait()
    bounds = [cus[0, d] for d in range(n_docs + 1)]

    def coords(t):
        seg = jnp.full(t.shape, bounds[0], jnp.int32)
        loc = jnp.full(t.shape, lax.div(bounds[0], cp), jnp.int32)
        plen = jnp.full(t.shape, lax.div(bounds[1] - bounds[0], 2 * cp), jnp.int32)
        for d in range(1, n_docs):
            first = lax.div(bounds[d], cp)
            hit = t >= first
            seg = jnp.where(hit, bounds[d], seg)
            loc = jnp.where(hit, first, loc)
            plen = jnp.where(hit, lax.div(bounds[d + 1] - bounds[d], 2 * cp), plen)
        within = t - loc
        up = within >= plen
        base = seg + within + jnp.where(up, (2 * cp - 2) * plen, 0)
        return seg, base, jnp.where(up, -plen, plen)

    _, key_base, key_slope = coords(t_row)
    lane_q = lax.broadcasted_iota(jnp.int32, (8, keys), 1)
    seg_q, base_q, slope_q = coords(lax.rem(lane_q, tok))
    rank_q = jnp.where(lane_q < tok, me, partner)
    pos_q = base_q + rank_q * slope_q
    lo_b = jnp.broadcast_to(seg_q[0:1], (tok, keys))
    hi_b = jnp.broadcast_to(pos_q[0:1], (tok, keys))

    def prepare(blk):
        s = SLOT[blk]
        for o in range(CORES):
            rank = chip_at(*blk) * CORES + (core if o == 0 else 1 - core)
            pos = key_base + rank * key_slope
            kf = kv[0, s, o].astype(jnp.float32)
            invalid = jnp.broadcast_to(kf[:, 0:1], (tok, keys)) == jnp.inf
            seen = (pos >= lo_b) & (pos <= hi_b) & jnp.logical_not(invalid)
            kaug[s, o * tok:(o + 1) * tok, 0:hd] = jnp.where(kf == jnp.inf, 0.0, kf).astype(jnp.bfloat16)
            kaug[s, o * tok:(o + 1) * tok, hd:2 * hd] = jnp.where(seen, 0.0, NEG).astype(jnp.bfloat16)

    c2 = scale * math.log2(math.e)

    def scores(group):
        lo, n = SLOT[group[0]], len(group)
        for blk in group:
            prepare(blk)
        s = dot(kaug[lo:lo + n].reshape(n * keys, 2 * hd), qt[...])
        sbuf[lo:lo + n] = s.reshape(n, keys, rows)

    def grads_p(group):
        lo, n = SLOT[group[0]], len(group)
        vb = kv[1, lo:lo + n].reshape(n * keys, hd)
        dpbuf[lo:lo + n] = dot(vb, dot_b[...]).reshape(n, keys, rows)

    def softmax(group, first):
        lo, n = SLOT[group[0]], len(group)
        mx = jnp.max(sbuf[lo:lo + n].reshape(n * keys, rows), axis=0, keepdims=True)
        if first:
            m_new = mx
        else:
            m_old = m_ref[...]
            m_new = jnp.maximum(m_old, mx)
            alpha = jnp.exp2((m_old - m_new) * c2)
        m_ref[...] = m_new
        mc = m_new * c2
        total = None
        for i in range(n):
            p = jnp.exp2(sbuf[lo + i] * c2 - mc)
            pbuf[lo + i] = p.astype(jnp.bfloat16)
            part_sum = jnp.sum(p, axis=0, keepdims=True)
            total = part_sum if total is None else total + part_sum
        pv = dot(kv[1, lo:lo + n].reshape(n * keys, hd), pbuf[lo:lo + n].reshape(n * keys, rows), TN)
        if first:
            l_ref[...] = total
            o_t[...] = pv
        else:
            l_ref[...] = l_ref[...] * alpha + total
            o_t[...] = o_t[...] * alpha + pv

    started = [False, False, False]
    for item in GATHER[early:]:
        if len(item) == 6:
            with scope('fwd%d_%d%d_%d' % item[:4]):
                forward(*item)
            continue
        gi, stage = item
        group = GROUPS[gi]
        with scope('wait%d_%d' % item):
            for blk in group:
                for o in range(CORES):
                    arrive(min(stage, 1), blk, o)
            if not started[0]:
                c_q.wait()
                x_q.wait_recv()
                qt[0:hd, :] = jnp.transpose(qbuf[...].reshape(rows, hd).astype(jnp.float32)).astype(jnp.bfloat16)
                started[0] = True
            if stage == 2 and not started[1]:
                c_do.wait()
                x_do.wait_recv()
                do_t = jnp.transpose(dob[...].reshape(rows, hd).astype(jnp.float32))
                dot_t[...] = do_t
                dot_b[...] = do_t.astype(jnp.bfloat16)
                started[1] = True
        with scope('group%d_%d' % item):
            if stage == 0:
                scores(group)
            elif stage == 1:
                softmax(group, not started[2])
                started[2] = True
            else:
                grads_p(group)

    scope_fin = scope('finish')
    scope_fin.__enter__()
    m_fin, l_fin = m_ref[...], l_ref[...]
    has_key = m_fin > NEG * 0.5
    safe = jnp.where(has_key, l_fin, 1.0)
    o_b = jnp.where(has_key, o_t[...] / safe, 0.0).astype(jnp.bfloat16).astype(jnp.float32)
    o_t[...] = o_b
    delta = jnp.sum(o_b * dot_t[...], axis=0, keepdims=True)
    lse = jnp.where(has_key, m_fin * scale + jnp.log(safe), 0.0)
    lse2 = jnp.where(has_key, m_fin * c2 + jnp.log2(safe), 0.0)

    scope_fin.__exit__(None, None, None)

    def rsend(X, blk, o, key, step):
        i = RIDX[key]
        push(part.at[X, SLOT[blk], o], rbuf.at[X, i], rs_send.at[X, i], rs_recv.at[X, i], nbr(unframe(X, *step)))

    def rwait(X, key):
        i = RIDX[key]
        remote(rbuf.at[X, i], rbuf.at[X, i], rs_send.at[X, i], rs_recv.at[X, i], to_partner).wait_recv()
        return rbuf[X, i]

    def total(X, a, b, o):
        s = SLOT[unframe(X, a, b)]
        keys_in = terms(a, b, o)
        if keys_in:
            acc = part[X, s, o]
            for key in keys_in:
                acc = acc + rwait(X, key)
            part[X, s, o] = acc

    def backward(blk):
        s = SLOT[blk]
        p = jnp.exp2(sbuf[s] * c2 - lse2)
        pbuf[s] = p.astype(jnp.bfloat16)
        dsbuf[s] = (p * (dpbuf[s] - delta)).astype(jnp.bfloat16)
        part[1, s] = dot(pbuf[s], dob[...].reshape(rows, hd)).reshape(CORES, tok, hd)
        part[0, s] = dot(dsbuf[s], qbuf[...].reshape(rows, hd)).reshape(CORES, tok, hd)

    x_out = []

    def store_o():
        o_rows = jnp.transpose(o_t[...]).astype(jnp.bfloat16).reshape(2 * grp, tok, hd)
        o_out[pl.ds(mine, grp)] = o_rows[0:grp]
        ost[...] = o_rows[grp:2 * grp]
        for h in range(grp):
            lse_out[core, h:h + 1, :] = lse[:, h * tok:(h + 1) * tok]
            lsest[h:h + 1, :] = lse[:, (grp + h) * tok:(grp + h + 1) * tok]
        x_out.append(push(ost, o_out.at[pl.ds(mine, grp)], pair_send.at[4], pair_recv.at[4], to_partner))
        x_out.append(push(lsest, lse_out.at[core], pair_send.at[5], pair_recv.at[5], to_partner))

    def store_dq():
        dq_t = dot(kaug[:, :, 0:hd].reshape(NBLK * keys, hd), dsbuf[...].reshape(NBLK * keys, rows), TN)
        dq_rows = (jnp.transpose(dq_t) * scale).astype(jnp.bfloat16).reshape(2 * grp, tok, hd)
        dq_out[pl.ds(mine, grp)] = dq_rows[0:grp]
        dqst[...] = dq_rows[grp:2 * grp]
        x_out.append(push(dqst, dq_out.at[pl.ds(mine, grp)], pair_send.at[6], pair_recv.at[6], to_partner))

    x_kv, owns = {}, {}

    def finish(X, o):
        total(X, 0, 0, o)
        res = part[X, 0, o] * scale if X == 0 else part[X, 0, o]
        if o == 1:
            kvsend[X] = res.astype(jnp.bfloat16)
            x_kv[X] = push(kvsend.at[X], kvrecv.at[X], pair_send.at[7 + X], pair_recv.at[7 + X], to_partner)
        else:
            owns[X] = res.astype(jnp.bfloat16).astype(jnp.float32)

    for item in SCATTER:
        if len(item) == 3:
            with scope('late%d_%d' % item[:2]):
                grads_p(GROUPS[item[0]])
        elif len(item) == 2:
            with scope('bwd%d%d' % item):
                backward(item)
        elif len(item) == 1:
            with scope('store%d' % item):
                (store_o, store_dq)[item[0]]()
        elif item[1:3] == (0, 0):
            with scope('final%d_%d' % (item[0], item[3])):
                finish(item[0], item[3])
        else:
            X, a, b, o = item
            with scope('sum%d_%d%d_%d' % item):
                total(X, a, b, o)
                step, key = target(a, b, o)
                rsend(X, unframe(X, a, b), o, key, step)

    scope_out = scope('tail')
    scope_out.__enter__()
    for X, out in ((0, dk_out), (1, dv_out)):
        x_kv[X].wait_recv()
        got = kvrecv[X].astype(jnp.float32)
        tmp32[X, pl.ds(0, tok, stride=2), :] = jnp.where(core == 0, owns[X], got)
        tmp32[X, pl.ds(1, tok, stride=2), :] = jnp.where(core == 0, got, owns[X])
        out[...] = tmp32[X].astype(jnp.bfloat16)
    for c in sends:
        c.wait_send()
    for x in x_out:
        x.wait_recv()
    scope_out.__exit__(None, None, None)


def store_kernel(o_in, lse_in, dq_in, dk_in, dv_in, o_out, lse_out, dq_out, dk_out, dv_out, lse_v, sem):
    copies = [pltpu.make_async_copy(a, b, sem.at[i]) for i, (a, b) in enumerate(
        ((o_in, o_out), (dq_in, dq_out), (dk_in, dk_out), (dv_in, dv_out), (lse_v, lse_out)))]
    for c in copies[:4]:
        c.start()
    grp = lse_in.shape[1]
    for i in range(lse_in.shape[0]):
        lse_v[i * grp:(i + 1) * grp, :] = lse_in[i]
    copies[4].start()
    for c in copies:
        c.wait()


def solution(mesh):
    cp = mesh.shape['cp']
    tok_spec = P(('dp', 'cp'), None, None)

    def local(q, k, v, do, valid, cu):
        tok, heads, hd = q.shape
        kvh = k.shape[1]
        grp = heads // kvh
        n_docs = cu.shape[0] - 1
        rows = CORES * grp * tok
        keys = CORES * tok
        assert kvh == CORES and cp == CORES * SIDE * SIDE and keys == hd
        bf, f32 = jnp.bfloat16, jnp.float32
        hbm_spec = pl.BlockSpec(memory_space=pltpu.HBM)
        vmem_spec = pl.BlockSpec(memory_space=pltpu.VMEM)
        n_rs = len(RIDX)
        flat = lambda x: x.reshape(tok * kvh, hd)
        o, lse, dq, dk, dv = pl.pallas_call(
            functools.partial(kernel, cp, n_docs, hd ** -0.5),
            name='ring_attention',
            out_shape=[
                jax.ShapeDtypeStruct((heads, tok, hd), bf),
                jax.ShapeDtypeStruct((CORES, grp, tok), f32),
                jax.ShapeDtypeStruct((heads, tok, hd), bf),
                jax.ShapeDtypeStruct((tok * kvh, hd), bf),
                jax.ShapeDtypeStruct((tok * kvh, hd), bf),
            ],
            in_specs=[hbm_spec] * 6,
            out_specs=[vmem_spec] * 5,
            scratch_shapes=[
                pltpu.VMEM((2, tok * kvh, hd), bf),
                pltpu.VMEM((2, tok * kvh, hd), f32),
                pltpu.VMEM((2, tok, hd), bf),
                pltpu.VMEM((2, NBLK, CORES, tok, hd), bf),
                pltpu.VMEM((NBLK, keys, 2 * hd), bf),
                pltpu.VMEM((CORES * grp, tok, hd), bf),
                pltpu.VMEM((hd + keys, rows), bf),
                pltpu.VMEM((CORES * grp, tok, hd), bf),
                pltpu.VMEM((hd, rows), f32),
                pltpu.VMEM((hd, rows), bf),
                pltpu.VMEM((NBLK, keys, rows), f32),
                pltpu.VMEM((NBLK, keys, rows), f32),
                pltpu.VMEM((NBLK, keys, rows), bf),
                pltpu.VMEM((NBLK, keys, rows), bf),
                pltpu.VMEM((2, NBLK, CORES, tok, hd), f32),
                pltpu.VMEM((2, n_rs, tok, hd), f32),
                pltpu.VMEM((grp, tok, hd), bf),
                pltpu.VMEM((grp, tok, hd), bf),
                pltpu.VMEM((grp, tok), f32),
                pltpu.VMEM((2, tok, hd), bf),
                pltpu.VMEM((2, tok, hd), bf),
                pltpu.VMEM((2, tok * kvh, hd), f32),
                pltpu.VMEM((1, rows), f32),
                pltpu.VMEM((1, rows), f32),
                pltpu.VMEM((hd, rows), f32),
                pltpu.VMEM((1, tok), jnp.int32),
                pltpu.SMEM((1, n_docs + 1), jnp.int32),
                pltpu.SemaphoreType.DMA((6,)),
                pltpu.SemaphoreType.DMA((9,)),
                pltpu.SemaphoreType.DMA((9,)),
                pltpu.SemaphoreType.DMA((64,)),
                pltpu.SemaphoreType.DMA((2, NBLK, CORES)),
                pltpu.SemaphoreType.DMA((2, n_rs)),
                pltpu.SemaphoreType.DMA((2, n_rs)),
            ],
            compiler_params=pltpu.CompilerParams(
                collective_id=0, has_side_effects=True, vmem_limit_bytes=40 * 1024 * 1024),
        )(*(pltpu.with_memory_space_constraint(a, pltpu.HBM) for a in (q.transpose(1, 0, 2), flat(k), flat(v), do.transpose(1, 0, 2), valid.reshape(1, tok), cu.reshape(1, n_docs + 1))))
        o, lse, dq, dk, dv = pl.pallas_call(
            store_kernel,
            name='store_outputs',
            out_shape=[
                jax.ShapeDtypeStruct((heads, tok, hd), bf),
                jax.ShapeDtypeStruct((heads, tok), f32),
                jax.ShapeDtypeStruct((heads, tok, hd), bf),
                jax.ShapeDtypeStruct((tok * kvh, hd), bf),
                jax.ShapeDtypeStruct((tok * kvh, hd), bf),
            ],
            in_specs=[vmem_spec] * 5,
            out_specs=[hbm_spec] * 5,
            scratch_shapes=[pltpu.VMEM((heads, tok), f32), pltpu.SemaphoreType.DMA((5,))],
            compiler_params=pltpu.CompilerParams(vmem_limit_bytes=1024 * 1024),
        )(o, lse, dq, dk, dv)
        back = lambda x: x.reshape(tok, kvh, hd)
        return (o.transpose(1, 0, 2), lse.transpose(1, 0), dq.transpose(1, 0, 2), back(dk), back(dv))

    return jax.shard_map(
        local, mesh=mesh,
        in_specs=(tok_spec, tok_spec, tok_spec, tok_spec, P(('dp', 'cp')), P('dp')),
        out_specs=(tok_spec, P(('dp', 'cp'), None), tok_spec, tok_spec, tok_spec), check_vma=False)
```

```python
import functools
import math

import jax
import jax.numpy as jnp
from jax import lax
from jax.experimental import pallas as pl
from jax.experimental.pallas import tpu as pltpu
from jax.sharding import PartitionSpec as P

MESH = pl.DeviceIdType.MESH
scope = jax.named_scope
NEG = -(2.0 ** 126)
CORES = 2
SIDE = 4
GROUPS = (
    ((0, 0),),
    ((1, 0), (3, 0), (0, 1), (0, 3)),
    ((1, 1), (1, 3), (3, 1), (3, 3)),
    ((2, 0), (0, 2)),
    ((2, 1), (2, 3), (1, 2), (3, 2)),
    ((2, 2),),
)
BLOCKS = tuple(blk for group in GROUPS for blk in group)
SLOT = {blk: i for i, blk in enumerate(BLOCKS)}
NBLK = len(BLOCKS)
ORDER = (
    (0, 0, 0, 0, 1, 0, 2), (0, 1, 0, 0, 1, 0, 2), (0, 1, 0, 0, 0, 0, 2), (0, 0, 0, 0, 1, 0, 1), (0, 0, 0, 0, 0, 0, 2),
    (0, 1, 0, 0, 1, 0, 1), (0, 0, 0, 0, 0, 0, -1), (0, 1, 0, 0, 0, 0, 1), (0, 1, 0, 0, 1, 0, -1), (0, 1, 0, 0, 0, 0, -1),
    (0, 0, 0, 0, 0, 0, 1), (0, 0, 0, 0, 1, 0, -1), (1, 0, 0), (0, 0, 0, 0, 1, 1, 1), (0, 0, 0, 0, 1, 1, 2),
    (0, 0, 0, 0, 0, 1, 2), (0, 1, 0, 0, 0, 1, 2), (0, 1, 0, 0, 1, 1, -1), (0, 1, 0, 0, 1, 1, 2), (0, 0, 0, 0, 1, 1, -1),
    (1, 0, 1), (0, 1, 0, 0, 1, 1, 1), (0, 0, 0, 0, 0, 1, 1), (0, 1, 0, 0, 0, 1, 1), (0, 0, 0, 0, 0, 1, -1),
    (0, 1, 0, 0, 0, 1, -1), (0, 0, 2, 0, 1, 1, 2), (0, 0, 2, 0, 1, 1, -1), (0, 0, 2, 0, 1, 1, 1), (0, 1, 2, 0, 1, 1, -1),
    (0, 1, 2, 0, 1, 1, 2), (0, 0, 2, 0, 0, 1, 2), (0, 1, 2, 0, 0, 1, 2), (0, 1, 2, 0, 0, 1, -1), (0, 0, 2, 0, 0, 1, -1),
    (0, 1, 2, 0, 0, 1, 1), (0, 0, 2, 0, 0, 1, 1), (1, 0, 2), (0, 1, 2, 0, 1, 1, 1), (0, 0, 3, 0, 0, 1, 2),
    (0, 1, 3, 0, 1, 1, 2), (0, 0, 1, 0, 0, 1, 2), (0, 0, 3, 0, 1, 1, 2), (0, 1, 1, 0, 0, 1, 2), (0, 1, 3, 0, 0, 1, 2),
    (0, 1, 1, 0, 1, 1, 2), (0, 0, 1, 0, 1, 1, 2), (0, 1, 1, 0, 1, 1, -1), (1, 3, 0), (1, 3, 1),
    (1, 3, 2), (0, 0, 1, 0, 0, 1, -1), (0, 0, 3, 0, 1, 1, -1), (0, 0, 3, 0, 0, 1, -1), (0, 0, 3, 0, 0, 1, 1),
    (0, 0, 1, 0, 1, 1, -1), (0, 1, 3, 0, 0, 1, -1), (0, 0, 1, 0, 0, 1, 1), (0, 0, 3, 0, 1, 1, 1), (0, 0, 1, 0, 1, 1, 1),
    (1, 1, 2), (1, 1, 0), (0, 1, 1, 0, 0, 1, -1), (0, 1, 3, 0, 1, 1, 1), (0, 1, 3, 0, 1, 1, -1),
    (0, 1, 3, 0, 0, 1, 1), (0, 1, 1, 0, 1, 1, 1), (0, 1, 1, 0, 0, 1, 1), (1, 1, 1), (1, 5, 0),
    (1, 5, 2), (1, 5, 1), (1, 4, 0), (1, 4, 2), (1, 4, 1),
    (1, 2, 0), (1, 2, 1), (2, 0), (3, 2, 1), (4, 1, 1, 2, 1),
    (4, 0, 2, 1, 0), (4, 1, 1, 2, 0), (3, 2, 2), (4, 0, 2, 2, 0), (4, 1, 2, 2, 1),
    (4, 0, 2, 2, 1), (4, 1, 2, 2, 0), (3, 2, 3), (4, 0, 2, 3, 1), (4, 1, 3, 2, 0),
    (3, 1, 2), (4, 1, 3, 2, 1), (4, 0, 1, 2, 0), (4, 0, 1, 2, 1), (3, 3, 2),
    (4, 0, 3, 2, 1), (4, 1, 2, 3, 1), (4, 1, 2, 1, 0), (4, 0, 3, 2, 0), (3, 0, 3),
    (3, 0, 2), (3, 2, 0), (4, 1, 0, 2, 1), (4, 0, 0, 2, 1), (1, 2, 2),
    (3, 3, 3), (3, 1, 1), (4, 0, 0, 2, 0), (4, 1, 3, 3, 1), (4, 1, 1, 1, 0),
    (4, 1, 0, 2, 0), (3, 3, 1), (4, 0, 1, 1, 0), (4, 0, 2, 3, 0), (3, 1, 3),
    (4, 1, 3, 1, 0), (4, 1, 1, 3, 0), (4, 1, 2, 1, 1), (4, 1, 1, 1, 1), (4, 0, 2, 1, 1),
    (4, 0, 3, 3, 1), (4, 1, 3, 3, 0), (4, 1, 1, 3, 1), (4, 1, 2, 3, 0), (4, 0, 3, 1, 0),
    (4, 1, 3, 1, 1), (5, 0), (4, 0, 1, 3, 0), (3, 1, 0), (4, 0, 1, 1, 1),
    (3, 3, 0), (4, 0, 3, 3, 0), (4, 0, 3, 1, 1), (4, 0, 1, 3, 1), (3, 0, 0),
    (4, 0, 0, 3, 1), (3, 0, 1), (5, 1), (4, 0, 0, 3, 0), (4, 0, 0, 1, 1),
    (4, 0, 0, 1, 0), (4, 1, 0, 1, 1), (4, 1, 0, 3, 1), (4, 1, 0, 3, 0), (4, 1, 0, 1, 0),
    (4, 1, 3, 0, 0), (4, 1, 1, 0, 0), (4, 1, 1, 0, 1), (4, 0, 2, 0, 0), (4, 1, 2, 0, 0),
    (4, 0, 2, 0, 1), (4, 1, 2, 0, 1), (4, 0, 1, 0, 0), (4, 0, 3, 0, 0), (4, 0, 1, 0, 1),
    (4, 1, 3, 0, 1), (4, 0, 3, 0, 1), (4, 1, 0, 0, 1), (4, 0, 0, 0, 1), (4, 1, 0, 0, 0),
    (6, 0), (4, 0, 0, 0, 0), (6, 1),
)
NT = (((1,), (1,)), ((), ()))
TN = (((0,), (0,)), ((), ()))


def dot(a, b, dims=(((1,), (0,)), ((), ()))):
    return lax.dot_general(a, b, dims, preferred_element_type=jnp.float32)


def unframe(X, a, b):
    return (a, b) if X == 0 else (b, a)


def side(o):
    return -1 if o == 0 else 1


def terms(X, a, b, o):
    if b == 2:
        return []
    if b:
        return [('rb', a, o)] if side(o) == (-1 if b == 3 else 1) else []
    out = [('fb', a, o, 1), ('fb', a, o, -1)]
    if a == 0 and o == 0:
        out += [('fa', o, 1), ('fa', o, -1), ('ra', o)]
    return out


def target(X, a, b, o):
    if b == 2:
        return (0, side(o)), ('rb', a, o)
    if b:
        return (0, -1 if b == 3 else 1), ('fb', a, o, 1 if b == 3 else -1)
    if a == 2:
        return (2, 0), ('ra', o)
    return (-1 if a == 3 else 1, 0), ('fa', o, 1 if a == 3 else -1)


RIDX = {}
for _a in range(SIDE):
    for _b in range(SIDE):
        for _o in range(CORES):
            if (_a, _b) != (0, 0):
                RIDX[target(0, _a, _b, _o)[1]] = len(RIDX)


def kernel(cp, n_docs, scale, q_hbm, k_hbm, v_hbm, do_hbm, val_hbm, cu_hbm,
           o_out, lse_out, dq_out, dk_out, dv_out,
           kin, kf32, oth, kv, kaug, qbuf, qt, dob, dot_t, dot_b, sbuf, dpbuf, pbuf, dsbuf, part, rbuf,
           ost, dqst, lsest, last, grad, tmp32, m_ref, l_ref, lse_v, lse2_v, delta_v, top, o_t, valv, cus,
           loc_sem, pair_send, pair_recv, ag_send, ag_recv, rs_send, rs_recv):
    tok = valv.shape[1]
    grp = ost.shape[0]
    rows = CORES * grp * tok
    hd = kin.shape[-1]
    keys = CORES * tok
    me = lax.axis_index('cp')
    core = lax.rem(me, CORES)
    chip = lax.div(me, CORES)
    cx = lax.rem(chip, SIDE)
    cy = lax.div(chip, SIDE)
    partner = me + 1 - 2 * core

    def chip_at(dx, dy):
        return lax.rem(cy + dy + SIDE, SIDE) * SIDE + lax.rem(cx + dx + SIDE, SIDE)

    def nbr(step, cross=False):
        return {'cp': chip_at(*step) * CORES + (1 - core if cross else core)}

    mine = core * grp
    theirs = (1 - core) * grp
    to_partner = {'cp': partner}

    c_k = pltpu.make_async_copy(k_hbm, kin.at[0], loc_sem.at[0])
    c_v = pltpu.make_async_copy(v_hbm, kin.at[1], loc_sem.at[1])
    c_val = pltpu.make_async_copy(val_hbm, valv, loc_sem.at[2])
    c_cu = pltpu.make_async_copy(cu_hbm, cus, loc_sem.at[3])
    c_q = pltpu.make_async_copy(q_hbm.at[pl.ds(mine, grp)], qbuf.at[0:grp], loc_sem.at[4])
    c_do = pltpu.make_async_copy(do_hbm.at[pl.ds(mine, grp)], dob.at[0:grp], loc_sem.at[5])
    for c in (c_k, c_v, c_val, c_cu, c_q, c_do):
        c.start()

    barrier = pltpu.get_barrier_semaphore()
    near = ((1, 0), (-1, 0), (2, 0), (0, 1), (0, -1), (0, 2))
    peers = [to_partner] + [nbr(s, cross) for s in near for cross in (False, True)]
    for peer in peers:
        pl.semaphore_signal(barrier, inc=1, device_id=peer, device_id_type=MESH)

    sends = []

    def remote(src, dst, ssem, rsem, dev):
        copy = pltpu.make_async_remote_copy(src_ref=src, dst_ref=dst, send_sem=ssem, recv_sem=rsem,
                                            device_id=dev, device_id_type=MESH)
        return copy

    def push(src, dst, ssem, rsem, dev):
        copy = remote(src, dst, ssem, rsem, dev)
        copy.start()
        sends.append(copy)
        return copy

    with scope('load_kv'):
        for c in (c_k, c_v, c_val):
            c.wait()
    sub = lax.broadcasted_iota(jnp.int32, (tok, tok), 0)
    lane = lax.broadcasted_iota(jnp.int32, (tok, tok), 1)
    vcol = jnp.sum(jnp.where(sub == lane, jnp.broadcast_to(valv[...], (tok, tok)), 0), axis=1, keepdims=True)
    lane0 = lax.broadcasted_iota(jnp.int32, (tok, hd), 1) == 0
    bad = lane0 & (jnp.broadcast_to(vcol, (tok, hd)) <= 0)
    for X in range(2):
        kf32[X] = kin[X].astype(jnp.float32)
    for X in range(2):
        h0 = kf32[X, pl.ds(0, tok, stride=2), :]
        h1 = kf32[X, pl.ds(1, tok, stride=2), :]
        own = jnp.where(core == 0, h0, h1)
        other = jnp.where(core == 0, h1, h0)
        if X == 0:
            own = jnp.where(bad, jnp.inf, own)
            other = jnp.where(bad, jnp.inf, other)
        kv[X, 0, 0] = own.astype(jnp.bfloat16)
        oth[X] = other.astype(jnp.bfloat16)

    with scope('barrier'):
        pl.semaphore_wait(barrier, len(peers))

    here = {(X, (0, 0), 0) for X in range(2)}
    ag_count = [0]

    def arrive(X, blk, o):
        if (X, blk, o) not in here:
            s = SLOT[blk]
            remote(kv.at[X, s, o], kv.at[X, s, o], ag_send.at[0], ag_recv.at[X, s, o], to_partner).wait_recv()
            here.add((X, blk, o))

    def forward(X, a, b, o, phase, step):
        blk = unframe(X, a, b)
        step = unframe(X, step * (1 - phase), step * phase)
        cross = blk == (0, 0) and o == 1
        src = oth.at[X] if cross else kv.at[X, SLOT[blk], o]
        if not cross:
            arrive(X, blk, o)
        d = SLOT[(blk[0] - step[0]) % SIDE, (blk[1] - step[1]) % SIDE]
        push(src, kv.at[X, d, o], ag_send.at[ag_count[0]], ag_recv.at[X, d, o], nbr(step, cross))
        ag_count[0] += 1

    for X in range(2):
        push(oth.at[X], kv.at[X, 0, 1], pair_send.at[X], ag_recv.at[X, 0, 1], to_partner)
    early = 0
    while ORDER[early][0] == 0 and ORDER[early][2:4] == (0, 0):
        forward(*ORDER[early][1:])
        early += 1
    x_q = push(q_hbm.at[pl.ds(theirs, grp)], qbuf.at[grp:2 * grp], pair_send.at[2], pair_recv.at[2], to_partner)
    x_do = push(do_hbm.at[pl.ds(theirs, grp)], dob.at[grp:2 * grp], pair_send.at[3], pair_recv.at[3], to_partner)

    t_row = lax.broadcasted_iota(jnp.int32, (tok, hd), 0)
    t_sub = lax.broadcasted_iota(jnp.int32, (keys, rows), 0)
    t_lane = lax.broadcasted_iota(jnp.int32, (keys, rows), 1)
    token = lax.rem(t_lane, tok) + jnp.where(t_lane >= grp * tok, tok, 0)
    qt[hd:hd + keys, :] = jnp.where(t_sub == token, 1.0, 0.0).astype(jnp.bfloat16)

    with scope('wait_cu'):
        c_cu.wait()
    bounds = [cus[0, d] for d in range(n_docs + 1)]

    def coords(t):
        seg = jnp.full(t.shape, bounds[0], jnp.int32)
        loc = jnp.full(t.shape, lax.div(bounds[0], cp), jnp.int32)
        plen = jnp.full(t.shape, lax.div(bounds[1] - bounds[0], 2 * cp), jnp.int32)
        for d in range(1, n_docs):
            first = lax.div(bounds[d], cp)
            hit = t >= first
            seg = jnp.where(hit, bounds[d], seg)
            loc = jnp.where(hit, first, loc)
            plen = jnp.where(hit, lax.div(bounds[d + 1] - bounds[d], 2 * cp), plen)
        within = t - loc
        up = within >= plen
        base = seg + within + jnp.where(up, (2 * cp - 2) * plen, 0)
        return seg, base, jnp.where(up, -plen, plen)

    _, key_base, key_slope = coords(t_row)
    lane_q = lax.broadcasted_iota(jnp.int32, (8, keys), 1)
    seg_q, base_q, slope_q = coords(lax.rem(lane_q, tok))
    rank_q = jnp.where(lane_q < tok, me, partner)
    pos_q = base_q + rank_q * slope_q
    lo_b = jnp.broadcast_to(seg_q[0:1], (tok, keys))
    hi_b = jnp.broadcast_to(pos_q[0:1], (tok, keys))

    def prepare(blk):
        s = SLOT[blk]
        for o in range(CORES):
            rank = chip_at(*blk) * CORES + (core if o == 0 else 1 - core)
            pos = key_base + rank * key_slope
            kf = kv[0, s, o].astype(jnp.float32)
            invalid = jnp.broadcast_to(kf[:, 0:1], (tok, keys)) == jnp.inf
            seen = (pos >= lo_b) & (pos <= hi_b) & jnp.logical_not(invalid)
            kaug[s, o * tok:(o + 1) * tok, 0:hd] = jnp.where(kf == jnp.inf, 0.0, kf).astype(jnp.bfloat16)
            kaug[s, o * tok:(o + 1) * tok, hd:2 * hd] = jnp.where(seen, 0.0, NEG).astype(jnp.bfloat16)

    c2 = scale * math.log2(math.e)

    def scores(group):
        lo, n = SLOT[group[0]], len(group)
        for blk in group:
            prepare(blk)
        s = dot(kaug[lo:lo + n].reshape(n * keys, 2 * hd), qt[...])
        sbuf[lo:lo + n] = s.reshape(n, keys, rows)
        top[lo:lo + 1] = jnp.max(s, axis=0, keepdims=True)

    def grads_p(group):
        lo, n = SLOT[group[0]], len(group)
        vb = kv[1, lo:lo + n].reshape(n * keys, hd)
        dpbuf[lo:lo + n] = dot(vb, dot_b[...]).reshape(n, keys, rows)

    def softmax(group, first):
        lo, n = SLOT[group[0]], len(group)
        mx = top[lo:lo + 1]
        if first:
            m_new = mx
        else:
            m_old = m_ref[...]
            m_new = jnp.maximum(m_old, mx)
            alpha = jnp.exp2((m_old - m_new) * c2)
        m_ref[...] = m_new
        mc = m_new * c2
        total = None
        for i in range(n):
            p = jnp.exp2(sbuf[lo + i] * c2 - mc)
            pbuf[lo + i] = p.astype(jnp.bfloat16)
            part_sum = jnp.sum(p, axis=0, keepdims=True)
            total = part_sum if total is None else total + part_sum
        pv = dot(kv[1, lo:lo + n].reshape(n * keys, hd), pbuf[lo:lo + n].reshape(n * keys, rows), TN)
        if first:
            l_ref[...] = total
            o_t[...] = pv
        else:
            l_ref[...] = l_ref[...] * alpha + total
            o_t[...] = o_t[...] * alpha + pv

    def row_terms():
        m_fin, l_fin = m_ref[...], l_ref[...]
        has_key = m_fin > NEG * 0.5
        safe = jnp.where(has_key, l_fin, 1.0)
        o_b = jnp.where(has_key, o_t[...] / safe, 0.0).astype(jnp.bfloat16).astype(jnp.float32)
        o_t[...] = o_b
        delta_v[...] = jnp.sum(o_b * dot_t[...], axis=0, keepdims=True)
        lse_v[...] = jnp.where(has_key, m_fin * scale + jnp.log(safe), 0.0)
        lse2_v[...] = jnp.where(has_key, m_fin * c2 + jnp.log2(safe), 0.0)

    def rsend(X, a, b, o):
        step, key = target(X, a, b, o)
        i = RIDX[key]
        dev = nbr(unframe(X, *step), b == 0 and o == 1)
        push(part.at[X, SLOT[unframe(X, a, b)], o], rbuf.at[X, i], rs_send.at[X, i], rs_recv.at[X, i], dev)

    def rwait(X, key):
        i = RIDX[key]
        remote(rbuf.at[X, i], rbuf.at[X, i], rs_send.at[X, i], rs_recv.at[X, i], to_partner).wait_recv()
        return rbuf[X, i]

    def total(X, a, b, o):
        s = SLOT[unframe(X, a, b)]
        names = terms(X, a, b, o)
        if names:
            acc = part[X, s, o]
            for name in names:
                acc = acc + rwait(X, name)
            part[X, s, o] = acc

    def backward(blk):
        s = SLOT[blk]
        p = jnp.exp2(sbuf[s] * c2 - lse2_v[...])
        pbuf[s] = p.astype(jnp.bfloat16)
        dsbuf[s] = (p * (dpbuf[s] - delta_v[...])).astype(jnp.bfloat16)
        part[1, s] = dot(pbuf[s], dob[...].reshape(rows, hd)).reshape(CORES, tok, hd)
        part[0, s] = dot(dsbuf[s], qbuf[...].reshape(rows, hd)).reshape(CORES, tok, hd)

    x_out = []

    def store_o():
        o_rows = jnp.transpose(o_t[...]).astype(jnp.bfloat16).reshape(2 * grp, tok, hd)
        o_out[pl.ds(mine, grp)] = o_rows[0:grp]
        ost[...] = o_rows[grp:2 * grp]
        for h in range(grp):
            lse_out[core, h:h + 1, :] = lse_v[:, h * tok:(h + 1) * tok]
            lsest[h:h + 1, :] = lse_v[:, (grp + h) * tok:(grp + h + 1) * tok]
        x_out.append(push(ost, o_out.at[pl.ds(mine, grp)], pair_send.at[4], pair_recv.at[4], to_partner))
        x_out.append(push(lsest, lse_out.at[core], pair_send.at[5], pair_recv.at[5], to_partner))

    def store_dq():
        dq_t = dot(kaug[:, :, 0:hd].reshape(NBLK * keys, hd), dsbuf[...].reshape(NBLK * keys, rows), TN)
        dq_rows = (jnp.transpose(dq_t) * scale).astype(jnp.bfloat16).reshape(2 * grp, tok, hd)
        dq_out[pl.ds(mine, grp)] = dq_rows[0:grp]
        dqst[...] = dq_rows[grp:2 * grp]
        x_out.append(push(dqst, dq_out.at[pl.ds(mine, grp)], pair_send.at[6], pair_recv.at[6], to_partner))

    x_sum = {}

    def finish(X, o):
        total(X, 0, 0, o)
        if o == 1:
            x_sum[X] = push(part.at[X, 0, 1], last.at[X], pair_send.at[7 + X], pair_recv.at[7 + X], to_partner)
        else:
            grad[X, 0] = part[X, 0, 0] * scale if X == 0 else part[X, 0, 0]

    def finish_other(X):
        x_sum[X].wait_recv()
        acc = last[X]
        for name in (('fa', 1, 1), ('fa', 1, -1), ('ra', 1)):
            acc = acc + rwait(X, name)
        grad[X, 1] = acc * scale if X == 0 else acc

    def need_q():
        if 'q' not in ready:
            ready.add('q')
            c_q.wait()
            x_q.wait_recv()
            qt[0:hd, :] = jnp.transpose(qbuf[...].reshape(rows, hd).astype(jnp.float32)).astype(jnp.bfloat16)

    def need_do():
        if 'do' not in ready:
            ready.add('do')
            c_do.wait()
            x_do.wait_recv()
            do_t = jnp.transpose(dob[...].reshape(rows, hd).astype(jnp.float32))
            dot_t[...] = do_t
            dot_b[...] = do_t.astype(jnp.bfloat16)

    def group_part(gi, stage):
        group = GROUPS[gi]
        first = stage not in ready
        ready.add(stage)
        with scope('wait%d_%d' % (gi, stage)):
            for blk in group:
                for o in range(CORES):
                    arrive(min(stage, 1), blk, o)
            if stage == 0:
                need_q()
            elif stage == 2:
                need_do()
        with scope('group%d_%d' % (gi, stage)):
            if stage == 0:
                scores(group)
            elif stage == 1:
                softmax(group, first)
            else:
                grads_p(group)

    def pass_on(X, a, b, o):
        if (a, b) == (0, 0):
            finish(X, o)
        else:
            total(X, a, b, o)
            rsend(X, a, b, o)

    ready = set()
    for code, *item in ORDER[early:]:
        with scope('%d_' % code + '_'.join(map(str, item))):
            if code == 0:
                forward(*item)
            elif code == 1:
                group_part(*item)
            elif code == 2:
                need_do()
                row_terms()
            elif code == 3:
                backward(tuple(item))
            elif code == 4:
                pass_on(*item)
            elif code == 5:
                (store_o, store_dq)[item[0]]()
            else:
                finish_other(*item)

    scope_out = scope('tail')
    scope_out.__enter__()
    for X, out in ((0, dk_out), (1, dv_out)):
        own, other = grad[X, 0], grad[X, 1]
        tmp32[X, pl.ds(0, tok, stride=2), :] = jnp.where(core == 0, own, other)
        tmp32[X, pl.ds(1, tok, stride=2), :] = jnp.where(core == 0, other, own)
        out[...] = tmp32[X].astype(jnp.bfloat16)
    for c in sends:
        c.wait_send()
    for x in x_out:
        x.wait_recv()
    scope_out.__exit__(None, None, None)


def store_kernel(o_in, lse_in, dq_in, dk_in, dv_in, o_out, lse_out, dq_out, dk_out, dv_out, lse_v, sem):
    copies = [pltpu.make_async_copy(a, b, sem.at[i]) for i, (a, b) in enumerate(
        ((o_in, o_out), (dq_in, dq_out), (dk_in, dk_out), (dv_in, dv_out), (lse_v, lse_out)))]
    for c in copies[:4]:
        c.start()
    grp = lse_in.shape[1]
    for i in range(lse_in.shape[0]):
        lse_v[i * grp:(i + 1) * grp, :] = lse_in[i]
    copies[4].start()
    for c in copies:
        c.wait()


def solution(mesh):
    cp = mesh.shape['cp']
    tok_spec = P(('dp', 'cp'), None, None)

    def local(q, k, v, do, valid, cu):
        tok, heads, hd = q.shape
        kvh = k.shape[1]
        grp = heads // kvh
        n_docs = cu.shape[0] - 1
        rows = CORES * grp * tok
        keys = CORES * tok
        assert kvh == CORES and cp == CORES * SIDE * SIDE and keys == hd
        bf, f32 = jnp.bfloat16, jnp.float32
        hbm_spec = pl.BlockSpec(memory_space=pltpu.HBM)
        vmem_spec = pl.BlockSpec(memory_space=pltpu.VMEM)
        n_rs = len(RIDX)
        flat = lambda x: x.reshape(tok * kvh, hd)
        o, lse, dq, dk, dv = pl.pallas_call(
            functools.partial(kernel, cp, n_docs, hd ** -0.5),
            name='ring_attention',
            out_shape=[
                jax.ShapeDtypeStruct((heads, tok, hd), bf),
                jax.ShapeDtypeStruct((CORES, grp, tok), f32),
                jax.ShapeDtypeStruct((heads, tok, hd), bf),
                jax.ShapeDtypeStruct((tok * kvh, hd), bf),
                jax.ShapeDtypeStruct((tok * kvh, hd), bf),
            ],
            in_specs=[hbm_spec] * 6,
            out_specs=[vmem_spec] * 5,
            scratch_shapes=[
                pltpu.VMEM((2, tok * kvh, hd), bf),
                pltpu.VMEM((2, tok * kvh, hd), f32),
                pltpu.VMEM((2, tok, hd), bf),
                pltpu.VMEM((2, NBLK, CORES, tok, hd), bf),
                pltpu.VMEM((NBLK, keys, 2 * hd), bf),
                pltpu.VMEM((CORES * grp, tok, hd), bf),
                pltpu.VMEM((hd + keys, rows), bf),
                pltpu.VMEM((CORES * grp, tok, hd), bf),
                pltpu.VMEM((hd, rows), f32),
                pltpu.VMEM((hd, rows), bf),
                pltpu.VMEM((NBLK, keys, rows), f32),
                pltpu.VMEM((NBLK, keys, rows), f32),
                pltpu.VMEM((NBLK, keys, rows), bf),
                pltpu.VMEM((NBLK, keys, rows), bf),
                pltpu.VMEM((2, NBLK, CORES, tok, hd), f32),
                pltpu.VMEM((2, n_rs, tok, hd), f32),
                pltpu.VMEM((grp, tok, hd), bf),
                pltpu.VMEM((grp, tok, hd), bf),
                pltpu.VMEM((grp, tok), f32),
                pltpu.VMEM((2, tok, hd), f32),
                pltpu.VMEM((2, 2, tok, hd), f32),
                pltpu.VMEM((2, tok * kvh, hd), f32),
                pltpu.VMEM((1, rows), f32),
                pltpu.VMEM((1, rows), f32),
                pltpu.VMEM((1, rows), f32),
                pltpu.VMEM((1, rows), f32),
                pltpu.VMEM((1, rows), f32),
                pltpu.VMEM((NBLK, rows), f32),
                pltpu.VMEM((hd, rows), f32),
                pltpu.VMEM((1, tok), jnp.int32),
                pltpu.SMEM((1, n_docs + 1), jnp.int32),
                pltpu.SemaphoreType.DMA((6,)),
                pltpu.SemaphoreType.DMA((9,)),
                pltpu.SemaphoreType.DMA((9,)),
                pltpu.SemaphoreType.DMA((64,)),
                pltpu.SemaphoreType.DMA((2, NBLK, CORES)),
                pltpu.SemaphoreType.DMA((2, n_rs)),
                pltpu.SemaphoreType.DMA((2, n_rs)),
            ],
            compiler_params=pltpu.CompilerParams(
                collective_id=0, has_side_effects=True, vmem_limit_bytes=40 * 1024 * 1024),
        )(*(pltpu.with_memory_space_constraint(a, pltpu.HBM) for a in (q.transpose(1, 0, 2), flat(k), flat(v), do.transpose(1, 0, 2), valid.reshape(1, tok), cu.reshape(1, n_docs + 1))))
        o, lse, dq, dk, dv = pl.pallas_call(
            store_kernel,
            name='store_outputs',
            out_shape=[
                jax.ShapeDtypeStruct((heads, tok, hd), bf),
                jax.ShapeDtypeStruct((heads, tok), f32),
                jax.ShapeDtypeStruct((heads, tok, hd), bf),
                jax.ShapeDtypeStruct((tok * kvh, hd), bf),
                jax.ShapeDtypeStruct((tok * kvh, hd), bf),
            ],
            in_specs=[vmem_spec] * 5,
            out_specs=[hbm_spec] * 5,
            scratch_shapes=[pltpu.VMEM((heads, tok), f32), pltpu.SemaphoreType.DMA((5,))],
            compiler_params=pltpu.CompilerParams(vmem_limit_bytes=1024 * 1024),
        )(o, lse, dq, dk, dv)
        back = lambda x: x.reshape(tok, kvh, hd)
        return (o.transpose(1, 0, 2), lse.transpose(1, 0), dq.transpose(1, 0, 2), back(dk), back(dv))

    return jax.shard_map(
        local, mesh=mesh,
        in_specs=(tok_spec, tok_spec, tok_spec, tok_spec, P(('dp', 'cp')), P('dp')),
        out_specs=(tok_spec, P(('dp', 'cp'), None), tok_spec, tok_spec, tok_spec), check_vma=False)
```

```python
import functools
import math

import jax
import jax.numpy as jnp
from jax import lax
from jax.experimental import pallas as pl
from jax.experimental.pallas import tpu as pltpu
from jax.sharding import PartitionSpec as P

MESH = pl.DeviceIdType.MESH
scope = jax.named_scope
NEG = -(2.0 ** 126)
CORES = 2
SIDE = 4
GROUPS = (
    ((0, 0),),
    ((1, 0), (3, 0), (0, 1), (0, 3)),
    ((1, 1), (1, 3), (3, 1), (3, 3)),
    ((2, 0), (0, 2)),
    ((2, 1), (2, 3), (1, 2), (3, 2)),
    ((2, 2),),
)
BLOCKS = tuple(blk for group in GROUPS for blk in group)
SLOT = {blk: i for i, blk in enumerate(BLOCKS)}
NBLK = len(BLOCKS)


def all_tasks():
    far = (2, 1, 3, 0)
    tasks = []
    for X in range(2):
        for o in range(CORES):
            tasks += [(0, X, 0, 0, o, 0, step) for step in (1, -1, 2)]
            for a in range(SIDE):
                for step in (1, -1, 2):
                    if step == 2 and a in RELAYED:
                        tasks.append((0, X, a, 3 if o == 0 else 1, o, 1, 1 if o == 0 else -1))
                    else:
                        tasks.append((0, X, a, 0, o, 1, step))
    tasks += [(1, g, stage) for g in range(len(GROUPS)) for stage in range(3)] + [(2, 0)]
    tasks += [(3,) + blk for blk in BLOCKS] + [(5, 0), (5, 1)]
    for X in range(2):
        for o in range(CORES):
            tasks += [(4, X, a, b, o) for b in far for a in far]
        tasks.append((6, X))
    return tasks


RELAYED = ()
ORDER = tuple(all_tasks()[i] for i in dict.fromkeys(b for n in (
    0x112f200f022d011e2e1f, 0x00103c12140523313213, 0x3d30032104221a191837, 0x380b29280a27093e360e,
    0x3b081d262c3517344546, 0x47071c0d0c162b061b15, 0x413f25393a2a3324404b, 0x4d4c484a4942434e5a93,
    0x65835e619271825b7984, 0x5c9462725d739a866353, 0x59589574445754649c87, 0x8556666955888b969775,
    0x7b8c9b8a67985f6a5076, 0x516b777a4f7c52606c78, 0x68999d8d89908f9f6d8e, 0x7d9e6e6f7ea07fa18091,
    0x8170a2a2a2a2a2a2a2a2,
) for b in n.to_bytes(10, 'big')))
NT = (((1,), (1,)), ((), ()))
TN = (((0,), (0,)), ((), ()))


def dot(a, b, dims=(((1,), (0,)), ((), ()))):
    return lax.dot_general(a, b, dims, preferred_element_type=jnp.float32)


def unframe(X, a, b):
    return (a, b) if X == 0 else (b, a)


def side(o):
    return -1 if o == 0 else 1


def terms(X, a, b, o):
    if b == 2:
        return []
    if b:
        return [('rb', a, o)] if side(o) == (-1 if b == 3 else 1) else []
    out = [('fb', a, o, 1), ('fb', a, o, -1)]
    if a == 0 and o == 0:
        out += [('fa', o, 1), ('fa', o, -1), ('ra', o)]
    return out


def target(X, a, b, o):
    if b == 2:
        return (0, side(o)), ('rb', a, o)
    if b:
        return (0, -1 if b == 3 else 1), ('fb', a, o, 1 if b == 3 else -1)
    if a == 2:
        return (2, 0), ('ra', o)
    return (-1 if a == 3 else 1, 0), ('fa', o, 1 if a == 3 else -1)


RIDX = {}
for _a in range(SIDE):
    for _b in range(SIDE):
        for _o in range(CORES):
            if (_a, _b) != (0, 0):
                RIDX[target(0, _a, _b, _o)[1]] = len(RIDX)
RIDX['lo', 1] = len(RIDX)


def consumer(key):
    if key[0] == 'rb':
        return key
    if key[0] == 'fb':
        return ('sum',) + key[1:3]
    return ('sum', 0, 0) if key[1] == 0 else ('other',)


RSEM, RNUM = {}, {}
for _key in RIDX:
    RSEM.setdefault(consumer(_key), len(RSEM))
    RNUM[consumer(_key)] = RNUM.get(consumer(_key), 0) + 1


def passes_on(X, blk):
    return unframe(X, *blk)[1] == 0 or (unframe(X, *blk)[1] != 2 and unframe(X, *blk)[0] in RELAYED)


ASEM, ANUM = {}, {}
for _X in range(2):
    for _g, _group in enumerate(GROUPS):
        for _blk in _group:
            for _o in range(CORES):
                if _blk != (0, 0) or _o == 1:
                    _name = (_X, _blk, _o) if passes_on(_X, _blk) else (_X, _g)
                    ASEM[_X, _blk, _o] = _name
                    ANUM[_name] = ANUM.get(_name, 0) + 1
AIDX = {name: i for i, name in enumerate(ANUM)}


def kernel(cp, n_docs, scale, q_hbm, k_hbm, v_hbm, do_hbm, val_hbm, cu_hbm,
           o_out, lse_out, dq_out, dk_out, dv_out,
           kin, kf32, oth, kv, kaug, qbuf, qt, dob, dot_t, dot_b, sbuf, dpbuf, pbuf, dsbuf, part, rbuf,
           ost, dqst, lsest, grad, tmp32, outb, lse_all, m_ref, l_ref, lse_v, lse2_v, delta_v, top, o_t, valv, cus,
           loc_sem, pair_send, pair_recv, ag_send, ag_recv, rs_send, rs_recv):
    tok = valv.shape[1]
    grp = ost.shape[0] // CORES
    rows = CORES * grp * tok
    hd = kin.shape[-1]
    keys = CORES * tok
    me = lax.axis_index('cp')
    core = lax.rem(me, CORES)
    chip = lax.div(me, CORES)
    cx = lax.rem(chip, SIDE)
    cy = lax.div(chip, SIDE)
    partner = me + 1 - 2 * core

    def chip_at(dx, dy):
        return lax.rem(cy + dy + SIDE, SIDE) * SIDE + lax.rem(cx + dx + SIDE, SIDE)

    def nbr(step, cross=False):
        return {'cp': chip_at(*step) * CORES + (1 - core if cross else core)}

    mine = core * grp
    theirs = (1 - core) * grp
    to_partner = {'cp': partner}

    barrier = pltpu.get_barrier_semaphore()
    near = ((1, 0), (-1, 0), (2, 0), (0, 1), (0, -1), (0, 2))
    peers = [to_partner] + [nbr(s, cross) for s in near for cross in (False, True)]
    for peer in peers:
        pl.semaphore_signal(barrier, inc=1, device_id=peer, device_id_type=MESH)

    c_k = pltpu.make_async_copy(k_hbm, kin.at[0], loc_sem.at[0])
    c_v = pltpu.make_async_copy(v_hbm, kin.at[1], loc_sem.at[0])
    c_kv = pltpu.make_async_copy(kin, kin, loc_sem.at[0])
    c_val = pltpu.make_async_copy(val_hbm, valv, loc_sem.at[1])
    c_cu = pltpu.make_async_copy(cu_hbm, cus, loc_sem.at[2])
    c_q = pltpu.make_async_copy(q_hbm.at[pl.ds(mine, grp)], qbuf.at[0:grp], loc_sem.at[3])
    c_do = pltpu.make_async_copy(do_hbm.at[pl.ds(mine, grp)], dob.at[0:grp], loc_sem.at[4])
    for c in (c_k, c_v, c_val, c_cu, c_q, c_do):
        c.start()

    def remote(src, dst, ssem, rsem, dev):
        copy = pltpu.make_async_remote_copy(src_ref=src, dst_ref=dst, send_sem=ssem, recv_sem=rsem,
                                            device_id=dev, device_id_type=MESH)
        return copy

    def push(src, dst, ssem, rsem, dev):
        copy = remote(src, dst, ssem, rsem, dev)
        copy.start()
        return copy

    with scope('load_kv'):
        for c in (c_kv, c_val):
            c.wait()
    sub = lax.broadcasted_iota(jnp.int32, (tok, tok), 0)
    lane = lax.broadcasted_iota(jnp.int32, (tok, tok), 1)
    vcol = jnp.sum(jnp.where(sub == lane, jnp.broadcast_to(valv[...], (tok, tok)), 0), axis=1, keepdims=True)
    lane0 = lax.broadcasted_iota(jnp.int32, (tok, hd), 1) == 0
    bad = lane0 & (jnp.broadcast_to(vcol, (tok, hd)) <= 0)
    for X in range(2):
        kf32[X] = kin[X].astype(jnp.float32)
    for X in range(2):
        h0 = kf32[X, pl.ds(0, tok, stride=2), :]
        h1 = kf32[X, pl.ds(1, tok, stride=2), :]
        own = jnp.where(core == 0, h0, h1)
        other = jnp.where(core == 0, h1, h0)
        if X == 0:
            own = jnp.where(bad, jnp.inf, own)
            other = jnp.where(bad, jnp.inf, other)
        kv[X, 0, 0] = own.astype(jnp.bfloat16)
        oth[X] = other.astype(jnp.bfloat16)

    with scope('barrier'):
        pl.semaphore_wait(barrier, len(peers))

    here = {(X, (0, 0), 0) for X in range(2)}

    def arrival(X, blk, o):
        return ag_recv.at[AIDX[ASEM[X, blk, o]]]

    def arrive(X, blk, o):
        if (X, blk, o) not in here:
            name = ASEM[X, blk, o]
            n = ANUM[name]
            ref = kv.at[0, 0, 0] if n == 1 else kv.at[0, 0:n // 2]
            remote(ref, ref, ag_send, arrival(X, blk, o), to_partner).wait_recv()
            here.update(k for k, v in ASEM.items() if v == name)

    def forward(X, a, b, o, phase, step):
        blk = unframe(X, a, b)
        step = unframe(X, step * (1 - phase), step * phase)
        cross = blk == (0, 0) and o == 1
        src = oth.at[X] if cross else kv.at[X, SLOT[blk], o]
        if not cross:
            arrive(X, blk, o)
        d = SLOT[(blk[0] - step[0]) % SIDE, (blk[1] - step[1]) % SIDE]
        d_blk = BLOCKS[d]
        push(src, kv.at[X, d, o], ag_send, arrival(X, d_blk, o), nbr(step, cross))

    for X in range(2):
        push(oth.at[X], kv.at[X, 0, 1], ag_send, arrival(X, (0, 0), 1), to_partner)
    early = 0
    while ORDER[early][0] == 0 and ORDER[early][2:4] == (0, 0):
        forward(*ORDER[early][1:])
        early += 1
    x_q = push(q_hbm.at[pl.ds(theirs, grp)], qbuf.at[grp:2 * grp], pair_send.at[0], pair_recv.at[0], to_partner)
    x_do = push(do_hbm.at[pl.ds(theirs, grp)], dob.at[grp:2 * grp], pair_send.at[0], pair_recv.at[1], to_partner)

    t_row = lax.broadcasted_iota(jnp.int32, (tok, hd), 0)
    t_sub = lax.broadcasted_iota(jnp.int32, (keys, rows), 0)
    t_lane = lax.broadcasted_iota(jnp.int32, (keys, rows), 1)
    token = lax.rem(t_lane, tok) + jnp.where(t_lane >= grp * tok, tok, 0)
    qt[hd:hd + keys, :] = jnp.where(t_sub == token, 1.0, 0.0).astype(jnp.bfloat16)

    with scope('wait_cu'):
        c_cu.wait()
    bounds = [cus[0, d] for d in range(n_docs + 1)]

    def coords(t):
        seg = jnp.full(t.shape, bounds[0], jnp.int32)
        loc = jnp.full(t.shape, lax.div(bounds[0], cp), jnp.int32)
        plen = jnp.full(t.shape, lax.div(bounds[1] - bounds[0], 2 * cp), jnp.int32)
        for d in range(1, n_docs):
            first = lax.div(bounds[d], cp)
            hit = t >= first
            seg = jnp.where(hit, bounds[d], seg)
            loc = jnp.where(hit, first, loc)
            plen = jnp.where(hit, lax.div(bounds[d + 1] - bounds[d], 2 * cp), plen)
        within = t - loc
        up = within >= plen
        base = seg + within + jnp.where(up, (2 * cp - 2) * plen, 0)
        return seg, base, jnp.where(up, -plen, plen)

    _, key_base, key_slope = coords(t_row)
    lane_q = lax.broadcasted_iota(jnp.int32, (8, keys), 1)
    seg_q, base_q, slope_q = coords(lax.rem(lane_q, tok))
    rank_q = jnp.where(lane_q < tok, me, partner)
    pos_q = base_q + rank_q * slope_q
    lo_b = jnp.broadcast_to(seg_q[0:1], (tok, keys))
    hi_b = jnp.broadcast_to(pos_q[0:1], (tok, keys))

    def prepare(blk):
        s = SLOT[blk]
        for o in range(CORES):
            rank = chip_at(*blk) * CORES + (core if o == 0 else 1 - core)
            pos = key_base + rank * key_slope
            kf = kv[0, s, o].astype(jnp.float32)
            invalid = jnp.broadcast_to(kf[:, 0:1], (tok, keys)) == jnp.inf
            seen = (pos >= lo_b) & (pos <= hi_b) & jnp.logical_not(invalid)
            kaug[s, o * tok:(o + 1) * tok, 0:hd] = jnp.where(kf == jnp.inf, 0.0, kf).astype(jnp.bfloat16)
            kaug[s, o * tok:(o + 1) * tok, hd:2 * hd] = jnp.where(seen, 0.0, NEG).astype(jnp.bfloat16)

    c2 = scale * math.log2(math.e)

    def scores(group):
        lo, n = SLOT[group[0]], len(group)
        for blk in group:
            prepare(blk)
        s = dot(kaug[lo:lo + n].reshape(n * keys, 2 * hd), qt[...])
        sbuf[lo:lo + n] = s.reshape(n, keys, rows)
        top[lo:lo + 1] = jnp.max(s, axis=0, keepdims=True)

    def grads_p(group):
        lo, n = SLOT[group[0]], len(group)
        vb = kv[1, lo:lo + n].reshape(n * keys, hd)
        dpbuf[lo:lo + n] = dot(vb, dot_b[...]).reshape(n, keys, rows)

    def softmax(group, first):
        lo, n = SLOT[group[0]], len(group)
        mx = top[lo:lo + 1]
        if first:
            m_new = mx
        else:
            m_old = m_ref[...]
            m_new = jnp.maximum(m_old, mx)
            alpha = jnp.exp2((m_old - m_new) * c2)
        m_ref[...] = m_new
        mc = m_new * c2
        total = None
        for i in range(n):
            p = jnp.exp2(sbuf[lo + i] * c2 - mc)
            pbuf[lo + i] = p.astype(jnp.bfloat16)
            part_sum = jnp.sum(p, axis=0, keepdims=True)
            total = part_sum if total is None else total + part_sum
        pv = dot(kv[1, lo:lo + n].reshape(n * keys, hd), pbuf[lo:lo + n].reshape(n * keys, rows), TN)
        if first:
            l_ref[...] = total
            o_t[...] = pv
        else:
            l_ref[...] = l_ref[...] * alpha + total
            o_t[...] = o_t[...] * alpha + pv

    def row_terms():
        m_fin, l_fin = m_ref[...], l_ref[...]
        has_key = m_fin > NEG * 0.5
        safe = jnp.where(has_key, l_fin, 1.0)
        o_b = jnp.where(has_key, o_t[...] / safe, 0.0).astype(jnp.bfloat16).astype(jnp.float32)
        o_t[...] = o_b
        delta_v[...] = jnp.sum(o_b * dot_t[...], axis=0, keepdims=True)
        lse_v[...] = jnp.where(has_key, m_fin * scale + jnp.log(safe), 0.0)
        lse2_v[...] = jnp.where(has_key, m_fin * c2 + jnp.log2(safe), 0.0)

    def rsend(X, a, b, o):
        step, key = target(X, a, b, o)
        i = RIDX[key]
        dev = nbr(unframe(X, *step), b == 0 and o == 1)
        push(part.at[X, SLOT[unframe(X, a, b)], o], rbuf.at[X, i], rs_send, rs_recv.at[X, RSEM[consumer(key)]], dev)

    def rwait(X, names):
        name = consumer(names[0])
        assert len(names) == RNUM[name]
        ref = rbuf.at[X, 0:len(names)]
        remote(ref, ref, rs_send, rs_recv.at[X, RSEM[name]], to_partner).wait_recv()
        return [rbuf[X, RIDX[key]] for key in names]

    def total(X, a, b, o):
        s = SLOT[unframe(X, a, b)]
        names = terms(X, a, b, o)
        if names:
            acc = part[X, s, o]
            for term in rwait(X, names):
                acc = acc + term
            part[X, s, o] = acc

    def backward(blk):
        s = SLOT[blk]
        p = jnp.exp2(sbuf[s] * c2 - lse2_v[...])
        pbuf[s] = p.astype(jnp.bfloat16)
        dsbuf[s] = (p * (dpbuf[s] - delta_v[...])).astype(jnp.bfloat16)
        part[1, s] = dot(pbuf[s], dob[...].reshape(rows, hd)).reshape(CORES, tok, hd)
        part[0, s] = dot(dsbuf[s], qbuf[...].reshape(rows, hd)).reshape(CORES, tok, hd)

    x_out, x_lse = [], []

    local = []

    def store(src, dst, i):
        c = pltpu.make_async_copy(src, dst, loc_sem.at[i])
        c.start()
        local.append(c)

    def store_o():
        ost[...] = jnp.transpose(o_t[...]).astype(jnp.bfloat16).reshape(2 * grp, tok, hd)
        for i in range(CORES):
            for h in range(grp):
                j = (i * grp + h) * tok
                lsest[i, h:h + 1, :] = lse_v[:, j:j + tok]
        store(ost.at[0:grp], o_out.at[pl.ds(mine, grp)], 0)
        x_out.append(push(ost.at[grp:2 * grp], o_out.at[pl.ds(mine, grp)], pair_send.at[0], pair_recv.at[2], to_partner))
        x_lse.append(push(lsest.at[1], lsest.at[2], pair_send.at[1], pair_recv.at[3], to_partner))

    def store_dq():
        dq_t = dot(kaug[:, :, 0:hd].reshape(NBLK * keys, hd), dsbuf[...].reshape(NBLK * keys, rows), TN)
        dqst[...] = (jnp.transpose(dq_t) * scale).astype(jnp.bfloat16).reshape(2 * grp, tok, hd)
        store(dqst.at[0:grp], dq_out.at[pl.ds(mine, grp)], 1)
        x_out.append(push(dqst.at[grp:2 * grp], dq_out.at[pl.ds(mine, grp)], pair_send.at[0], pair_recv.at[2], to_partner))

    def finish(X, o):
        total(X, 0, 0, o)
        if o == 1:
            key = ('lo', 1)
            push(part.at[X, 0, 1], rbuf.at[X, RIDX[key]], rs_send, rs_recv.at[X, RSEM[consumer(key)]], to_partner)
        else:
            grad[X, 0] = part[X, 0, 0] * scale if X == 0 else part[X, 0, 0]

    def finish_other(X):
        acc = sum(rwait(X, (('lo', 1), ('fa', 1, 1), ('fa', 1, -1), ('ra', 1))))
        grad[X, 1] = acc * scale if X == 0 else acc

    def need_q():
        if 'q' not in ready:
            ready.add('q')
            c_q.wait()
            x_q.wait_recv()
            qt[0:hd, :] = jnp.transpose(qbuf[...].reshape(rows, hd).astype(jnp.float32)).astype(jnp.bfloat16)

    def need_do():
        if 'do' not in ready:
            ready.add('do')
            c_do.wait()
            x_do.wait_recv()
            do_t = jnp.transpose(dob[...].reshape(rows, hd).astype(jnp.float32))
            dot_t[...] = do_t
            dot_b[...] = do_t.astype(jnp.bfloat16)

    def group_part(gi, stage):
        group = GROUPS[gi]
        first = stage not in ready
        ready.add(stage)
        with scope('wait%d_%d' % (gi, stage)):
            for blk in group:
                for o in range(CORES):
                    arrive(min(stage, 1), blk, o)
            if stage == 0:
                need_q()
            elif stage == 2:
                need_do()
        with scope('group%d_%d' % (gi, stage)):
            if stage == 0:
                scores(group)
            elif stage == 1:
                softmax(group, first)
            else:
                grads_p(group)

    def pass_on(X, a, b, o):
        if (a, b) == (0, 0):
            finish(X, o)
        else:
            total(X, a, b, o)
            rsend(X, a, b, o)

    ready = set()
    for code, *item in ORDER[early:]:
        with scope('%d_' % code + '_'.join(map(str, item))):
            if code == 0:
                forward(*item)
            elif code == 1:
                group_part(*item)
            elif code == 2:
                need_do()
                row_terms()
            elif code == 3:
                backward(tuple(item))
            elif code == 4:
                pass_on(*item)
            elif code == 5:
                (store_o, store_dq)[item[0]]()
            else:
                finish_other(*item)

    scope_out = scope('tail')
    scope_out.__enter__()
    x_lse[0].wait_recv()
    lse_all[0:grp] = jnp.where(core == 0, lsest[0], lsest[2])
    lse_all[grp:2 * grp] = jnp.where(core == 0, lsest[2], lsest[0])
    store(lse_all, lse_out, 4)
    for X, out in ((0, dk_out), (1, dv_out)):
        own, other = grad[X, 0], grad[X, 1]
        tmp32[X, pl.ds(0, tok, stride=2), :] = jnp.where(core == 0, own, other)
        tmp32[X, pl.ds(1, tok, stride=2), :] = jnp.where(core == 0, other, own)
        outb[X] = tmp32[X].astype(jnp.bfloat16)
        store(outb.at[X], out, 2 + X)
    for ref, sem in ((rbuf.at[0], ag_send), (rbuf, rs_send), (dpbuf.at[0], pair_send.at[0])):
        remote(ref, ref, sem, sem, to_partner).wait_send()
    x_lse[0].wait_send()
    remote(ost, ost, pair_send.at[0], pair_recv.at[2], to_partner).wait_recv()
    for c in local:
        c.wait()
    scope_out.__exit__(None, None, None)


def store_kernel(*refs):
    n = len(refs) // 2
    copies = [pltpu.make_async_copy(refs[i], refs[n + i], refs[-1].at[i]) for i in range(n)]
    for c in copies:
        c.start()
    for c in copies:
        c.wait()


def solution(mesh):
    cp = mesh.shape['cp']
    tok_spec = P(('dp', 'cp'), None, None)

    def local(q, k, v, do, valid, cu):
        tok, heads, hd = q.shape
        kvh = k.shape[1]
        grp = heads // kvh
        n_docs = cu.shape[0] - 1
        rows = CORES * grp * tok
        keys = CORES * tok
        assert kvh == CORES and cp == CORES * SIDE * SIDE and keys == hd
        bf, f32 = jnp.bfloat16, jnp.float32
        hbm_spec = pl.BlockSpec(memory_space=pltpu.HBM)
        any_spec = pl.BlockSpec(memory_space=pl.ANY)
        n_rs = len(RIDX)
        flat = lambda x: x.reshape(tok * kvh, hd)
        o, lse, dq, dk, dv = pl.pallas_call(
            functools.partial(kernel, cp, n_docs, hd ** -0.5),
            name='ring_attention',
            out_shape=[
                jax.ShapeDtypeStruct((heads, tok, hd), bf),
                jax.ShapeDtypeStruct((heads, tok), f32),
                jax.ShapeDtypeStruct((heads, tok, hd), bf),
                jax.ShapeDtypeStruct((tok * kvh, hd), bf),
                jax.ShapeDtypeStruct((tok * kvh, hd), bf),
            ],
            in_specs=[hbm_spec] * 6,
            out_specs=[any_spec] * 5,
            scratch_shapes=[
                pltpu.VMEM((2, tok * kvh, hd), bf),
                pltpu.VMEM((2, tok * kvh, hd), f32),
                pltpu.VMEM((2, tok, hd), bf),
                pltpu.VMEM((2, NBLK, CORES, tok, hd), bf),
                pltpu.VMEM((NBLK, keys, 2 * hd), bf),
                pltpu.VMEM((CORES * grp, tok, hd), bf),
                pltpu.VMEM((hd + keys, rows), bf),
                pltpu.VMEM((CORES * grp, tok, hd), bf),
                pltpu.VMEM((hd, rows), f32),
                pltpu.VMEM((hd, rows), bf),
                pltpu.VMEM((NBLK, keys, rows), f32),
                pltpu.VMEM((NBLK, keys, rows), f32),
                pltpu.VMEM((NBLK, keys, rows), bf),
                pltpu.VMEM((NBLK, keys, rows), bf),
                pltpu.VMEM((2, NBLK, CORES, tok, hd), f32),
                pltpu.VMEM((2, n_rs, tok, hd), f32),
                pltpu.VMEM((heads, tok, hd), bf),
                pltpu.VMEM((heads, tok, hd), bf),
                pltpu.VMEM((CORES + 1, grp, tok), f32),
                pltpu.VMEM((2, 2, tok, hd), f32),
                pltpu.VMEM((2, tok * kvh, hd), f32),
                pltpu.VMEM((2, tok * kvh, hd), bf),
                pltpu.VMEM((heads, tok), f32),
                pltpu.VMEM((1, rows), f32),
                pltpu.VMEM((1, rows), f32),
                pltpu.VMEM((1, rows), f32),
                pltpu.VMEM((1, rows), f32),
                pltpu.VMEM((1, rows), f32),
                pltpu.VMEM((NBLK, rows), f32),
                pltpu.VMEM((hd, rows), f32),
                pltpu.VMEM((1, tok), jnp.int32),
                pltpu.SMEM((1, n_docs + 1), jnp.int32),
                pltpu.SemaphoreType.DMA((5,)),
                pltpu.SemaphoreType.DMA((2,)),
                pltpu.SemaphoreType.DMA((4,)),
                pltpu.SemaphoreType.DMA(()),
                pltpu.SemaphoreType.DMA((len(AIDX),)),
                pltpu.SemaphoreType.DMA(()),
                pltpu.SemaphoreType.DMA((2, len(RSEM))),
            ],
            compiler_params=pltpu.CompilerParams(
                collective_id=0, has_side_effects=True, vmem_limit_bytes=40 * 1024 * 1024),
        )(*(pltpu.with_memory_space_constraint(a, pltpu.HBM) for a in (q.transpose(1, 0, 2), flat(k), flat(v), do.transpose(1, 0, 2), valid.reshape(1, tok), cu.reshape(1, n_docs + 1))))
        o, lse, dq, dk, dv = pl.pallas_call(
            store_kernel,
            name='store_outputs',
            out_shape=[
                jax.ShapeDtypeStruct((heads, tok, hd), bf),
                jax.ShapeDtypeStruct((heads, tok), f32),
                jax.ShapeDtypeStruct((heads, tok, hd), bf),
                jax.ShapeDtypeStruct((tok * kvh, hd), bf),
                jax.ShapeDtypeStruct((tok * kvh, hd), bf),
            ],
            in_specs=[any_spec] * 5,
            out_specs=[hbm_spec] * 5,
            scratch_shapes=[pltpu.SemaphoreType.DMA((5,))],
            compiler_params=pltpu.CompilerParams(vmem_limit_bytes=1024 * 1024),
        )(o, lse, dq, dk, dv)
        back = lambda x: x.reshape(tok, kvh, hd)
        return (o.transpose(1, 0, 2), lse.transpose(1, 0), dq.transpose(1, 0, 2), back(dk), back(dv))

    return jax.shard_map(
        local, mesh=mesh,
        in_specs=(tok_spec, tok_spec, tok_spec, tok_spec, P(('dp', 'cp')), P('dp')),
        out_specs=(tok_spec, P(('dp', 'cp'), None), tok_spec, tok_spec, tok_spec), check_vma=False)
```

```python
import functools
import math

import jax
import jax.numpy as jnp
from jax import lax
from jax.experimental import pallas as pl
from jax.experimental.pallas import tpu as pltpu
from jax.sharding import PartitionSpec as P

MESH = pl.DeviceIdType.MESH
scope = jax.named_scope
NEG = -(2.0 ** 126)
CORES = 2
SIDE = 4
GROUPS = (
    ((0, 0),),
    ((1, 0), (3, 0), (0, 1), (0, 3)),
    ((1, 1), (1, 3), (3, 1), (3, 3)),
    ((2, 0), (0, 2)),
    ((2, 1), (2, 3), (1, 2), (3, 2)),
    ((2, 2),),
)
BLOCKS = tuple(blk for group in GROUPS for blk in group)
SLOT = {blk: i for i, blk in enumerate(BLOCKS)}
NBLK = len(BLOCKS)


def all_tasks():
    far = (2, 1, 3, 0)
    tasks = []
    for X in range(2):
        for o in range(CORES):
            tasks += [(0, X, 0, 0, o, 0, step) for step in (1, -1, 2)]
            for a in range(SIDE):
                for step in (1, -1, 2):
                    if step == 2 and a in RELAYED:
                        tasks.append((0, X, a, 3 if o == 0 else 1, o, 1, 1 if o == 0 else -1))
                    else:
                        tasks.append((0, X, a, 0, o, 1, step))
    tasks += [(1, g, stage) for g in range(len(GROUPS)) for stage in range(3)] + [(2, 0)]
    tasks += [(3,) + blk for blk in BLOCKS] + [(5, 0), (5, 1)]
    for X in range(2):
        for o in range(CORES):
            tasks += [(4, X, a, b, o) for b in far for a in far]
        tasks.append((6, X))
    return tasks


RELAYED = ()
ORDER = tuple(all_tasks()[i] for i in dict.fromkeys(b for n in (
    0x112f02200f2e10002d01, 0x1f1e3e31052314320422, 0x03133021123c181a0829, 0x0b38090e282c26171d35,
    0x3d190a3b274536461b37, 0x47240c063a151c3f342b, 0x070d39252a164033414b, 0x4d4c48494a42434e5e71,
    0x9282615c72865a658362, 0x935d63739a5b79948459, 0x74586485954457567b54, 0x669b5296535576978a9c,
    0x7a87756a50986b697788, 0x8b674f518c7c9d997860, 0x9f7e7d899e7f8f68a06d, 0x8d906e8e6c6f5f80a191,
    0x81a27070707070707070,
) for b in n.to_bytes(10, 'big')))
NT = (((1,), (1,)), ((), ()))
TN = (((0,), (0,)), ((), ()))


def dot(a, b, dims=(((1,), (0,)), ((), ()))):
    return lax.dot_general(a, b, dims, preferred_element_type=jnp.float32)


def unframe(X, a, b):
    return (a, b) if X == 0 else (b, a)


def side(o):
    return -1 if o == 0 else 1


def terms(X, a, b, o):
    if b == 2:
        return []
    if b:
        return [('rb', a, o)] if side(o) == (-1 if b == 3 else 1) else []
    out = [('fb', a, o, 1), ('fb', a, o, -1)]
    if a == 0 and o == 0:
        out += [('fa', o, 1), ('fa', o, -1), ('ra', o)]
    return out


def target(X, a, b, o):
    if b == 2:
        return (0, side(o)), ('rb', a, o)
    if b:
        return (0, -1 if b == 3 else 1), ('fb', a, o, 1 if b == 3 else -1)
    if a == 2:
        return (2, 0), ('ra', o)
    return (-1 if a == 3 else 1, 0), ('fa', o, 1 if a == 3 else -1)


RIDX = {}
for _a in range(SIDE):
    for _b in range(SIDE):
        for _o in range(CORES):
            if (_a, _b) != (0, 0):
                RIDX[target(0, _a, _b, _o)[1]] = len(RIDX)
RIDX['lo', 1] = len(RIDX)


def consumer(key):
    if key[0] == 'rb':
        return key
    if key[0] == 'fb':
        return ('sum',) + key[1:3]
    return ('sum', 0, 0) if key[1] == 0 else ('other',)


RSEM, RNUM = {}, {}
for _key in RIDX:
    RSEM.setdefault(consumer(_key), len(RSEM))
    RNUM[consumer(_key)] = RNUM.get(consumer(_key), 0) + 1


def passes_on(X, blk):
    return unframe(X, *blk)[1] == 0 or (unframe(X, *blk)[1] != 2 and unframe(X, *blk)[0] in RELAYED)


ASEM, ANUM = {}, {}
for _X in range(2):
    for _g, _group in enumerate(GROUPS):
        for _blk in _group:
            for _o in range(CORES):
                if _blk != (0, 0) or _o == 1:
                    _name = (_X, _blk, _o) if passes_on(_X, _blk) else (_X, _g)
                    ASEM[_X, _blk, _o] = _name
                    ANUM[_name] = ANUM.get(_name, 0) + 1
AIDX = {name: i for i, name in enumerate(ANUM)}


def kernel(cp, n_docs, scale, q_hbm, k_hbm, v_hbm, do_hbm, val_hbm, cu_hbm,
           o_out, lse_out, dq_out, dk_out, dv_out,
           kin, kf32, oth, kv, kaug, qbuf, qt, dob, dot_t, dot_b, sbuf, dpbuf, pbuf, dsbuf, part, rbuf,
           ost, dqst, lsest, grad, tmp32, outb, lse_all, m_ref, l_ref, lse_v, lse2_v, delta_v, top, o_t, valv, cus,
           loc_sem, pair_send, pair_recv, ag_send, ag_recv, rs_send, rs_recv):
    tok = valv.shape[1]
    grp = ost.shape[0] // CORES
    rows = CORES * grp * tok
    hd = kin.shape[-1]
    keys = CORES * tok
    me = lax.axis_index('cp')
    core = lax.rem(me, CORES)
    chip = lax.div(me, CORES)
    cx = lax.rem(chip, SIDE)
    cy = lax.div(chip, SIDE)
    partner = me + 1 - 2 * core

    def chip_at(dx, dy):
        return lax.rem(cy + dy + SIDE, SIDE) * SIDE + lax.rem(cx + dx + SIDE, SIDE)

    def nbr(step, cross=False):
        return {'cp': chip_at(*step) * CORES + (1 - core if cross else core)}

    mine = core * grp
    theirs = (1 - core) * grp
    to_partner = {'cp': partner}

    barrier = pltpu.get_barrier_semaphore()
    near = ((1, 0), (-1, 0), (2, 0), (0, 1), (0, -1), (0, 2))
    peers = [to_partner] + [nbr(s, cross) for s in near for cross in (False, True)]
    for peer in peers:
        pl.semaphore_signal(barrier, inc=1, device_id=peer, device_id_type=MESH)

    c_k = pltpu.make_async_copy(k_hbm, kin.at[0], loc_sem.at[0])
    c_v = pltpu.make_async_copy(v_hbm, kin.at[1], loc_sem.at[0])
    c_kv = pltpu.make_async_copy(kin, kin, loc_sem.at[0])
    c_val = pltpu.make_async_copy(val_hbm, valv, loc_sem.at[1])
    c_cu = pltpu.make_async_copy(cu_hbm, cus, loc_sem.at[2])
    c_q = pltpu.make_async_copy(q_hbm.at[pl.ds(mine, grp)], qbuf.at[0:grp], loc_sem.at[3])
    c_do = pltpu.make_async_copy(do_hbm.at[pl.ds(mine, grp)], dob.at[0:grp], loc_sem.at[4])
    for c in (c_k, c_v, c_val, c_cu, c_q, c_do):
        c.start()

    def remote(src, dst, ssem, rsem, dev):
        copy = pltpu.make_async_remote_copy(src_ref=src, dst_ref=dst, send_sem=ssem, recv_sem=rsem,
                                            device_id=dev, device_id_type=MESH)
        return copy

    def push(src, dst, ssem, rsem, dev):
        copy = remote(src, dst, ssem, rsem, dev)
        copy.start()
        return copy

    with scope('load_kv'):
        for c in (c_kv, c_val):
            c.wait()
    sub = lax.broadcasted_iota(jnp.int32, (tok, tok), 0)
    lane = lax.broadcasted_iota(jnp.int32, (tok, tok), 1)
    vcol = jnp.sum(jnp.where(sub == lane, jnp.broadcast_to(valv[...], (tok, tok)), 0), axis=1, keepdims=True)
    lane0 = lax.broadcasted_iota(jnp.int32, (tok, hd), 1) == 0
    bad = lane0 & (jnp.broadcast_to(vcol, (tok, hd)) <= 0)
    for X in range(2):
        kf32[X] = kin[X].astype(jnp.float32)
    for X in range(2):
        h0 = kf32[X, pl.ds(0, tok, stride=2), :]
        h1 = kf32[X, pl.ds(1, tok, stride=2), :]
        own = jnp.where(core == 0, h0, h1)
        other = jnp.where(core == 0, h1, h0)
        if X == 0:
            own = jnp.where(bad, jnp.inf, own)
            other = jnp.where(bad, jnp.inf, other)
        kv[X, 0, 0] = own.astype(jnp.bfloat16)
        oth[X] = other.astype(jnp.bfloat16)

    with scope('barrier'):
        pl.semaphore_wait(barrier, len(peers))

    here = {(X, (0, 0), 0) for X in range(2)}

    def arrival(X, blk, o):
        return ag_recv.at[AIDX[ASEM[X, blk, o]]]

    def arrive(X, blk, o):
        if (X, blk, o) not in here:
            name = ASEM[X, blk, o]
            n = ANUM[name]
            ref = kv.at[0, 0, 0] if n == 1 else kv.at[0, 0:n // 2]
            remote(ref, ref, ag_send, arrival(X, blk, o), to_partner).wait_recv()
            here.update(k for k, v in ASEM.items() if v == name)

    def forward(X, a, b, o, phase, step):
        blk = unframe(X, a, b)
        step = unframe(X, step * (1 - phase), step * phase)
        cross = blk == (0, 0) and o == 1
        src = oth.at[X] if cross else kv.at[X, SLOT[blk], o]
        if not cross:
            arrive(X, blk, o)
        d = SLOT[(blk[0] - step[0]) % SIDE, (blk[1] - step[1]) % SIDE]
        d_blk = BLOCKS[d]
        push(src, kv.at[X, d, o], ag_send, arrival(X, d_blk, o), nbr(step, cross))

    for X in range(2):
        push(oth.at[X], kv.at[X, 0, 1], ag_send, arrival(X, (0, 0), 1), to_partner)
    early = 0
    while ORDER[early][0] == 0 and ORDER[early][2:4] == (0, 0):
        forward(*ORDER[early][1:])
        early += 1
    x_q = push(q_hbm.at[pl.ds(theirs, grp)], qbuf.at[grp:2 * grp], pair_send.at[0], pair_recv.at[0], to_partner)
    x_do = push(do_hbm.at[pl.ds(theirs, grp)], dob.at[grp:2 * grp], pair_send.at[0], pair_recv.at[1], to_partner)

    t_row = lax.broadcasted_iota(jnp.int32, (tok, hd), 0)
    t_sub = lax.broadcasted_iota(jnp.int32, (keys, rows), 0)
    t_lane = lax.broadcasted_iota(jnp.int32, (keys, rows), 1)
    token = lax.rem(t_lane, tok) + jnp.where(t_lane >= grp * tok, tok, 0)
    qt[hd:hd + keys, :] = jnp.where(t_sub == token, 1.0, 0.0).astype(jnp.bfloat16)

    with scope('wait_cu'):
        c_cu.wait()
    bounds = [cus[0, d] for d in range(n_docs + 1)]

    def coords(t):
        seg = jnp.full(t.shape, bounds[0], jnp.int32)
        loc = jnp.full(t.shape, lax.div(bounds[0], cp), jnp.int32)
        plen = jnp.full(t.shape, lax.div(bounds[1] - bounds[0], 2 * cp), jnp.int32)
        for d in range(1, n_docs):
            first = lax.div(bounds[d], cp)
            hit = t >= first
            seg = jnp.where(hit, bounds[d], seg)
            loc = jnp.where(hit, first, loc)
            plen = jnp.where(hit, lax.div(bounds[d + 1] - bounds[d], 2 * cp), plen)
        within = t - loc
        up = within >= plen
        base = seg + within + jnp.where(up, (2 * cp - 2) * plen, 0)
        return seg, base, jnp.where(up, -plen, plen)

    _, key_base, key_slope = coords(t_row)
    lane_q = lax.broadcasted_iota(jnp.int32, (8, keys), 1)
    seg_q, base_q, slope_q = coords(lax.rem(lane_q, tok))
    rank_q = jnp.where(lane_q < tok, me, partner)
    pos_q = base_q + rank_q * slope_q
    lo_b = jnp.broadcast_to(seg_q[0:1], (tok, keys))
    hi_b = jnp.broadcast_to(pos_q[0:1], (tok, keys))

    def prepare(blk):
        s = SLOT[blk]
        for o in range(CORES):
            rank = chip_at(*blk) * CORES + (core if o == 0 else 1 - core)
            pos = key_base + rank * key_slope
            kf = kv[0, s, o].astype(jnp.float32)
            invalid = jnp.broadcast_to(kf[:, 0:1], (tok, keys)) == jnp.inf
            seen = (pos >= lo_b) & (pos <= hi_b) & jnp.logical_not(invalid)
            kaug[s, o * tok:(o + 1) * tok, 0:hd] = jnp.where(kf == jnp.inf, 0.0, kf).astype(jnp.bfloat16)
            kaug[s, o * tok:(o + 1) * tok, hd:2 * hd] = jnp.where(seen, 0.0, NEG).astype(jnp.bfloat16)

    c2 = scale * math.log2(math.e)

    def scores(group):
        lo, n = SLOT[group[0]], len(group)
        for blk in group:
            prepare(blk)
        s = dot(kaug[lo:lo + n].reshape(n * keys, 2 * hd), qt[...])
        sbuf[lo:lo + n] = s.reshape(n, keys, rows)
        top[lo:lo + 1] = jnp.max(s, axis=0, keepdims=True)

    def grads_p(group):
        lo, n = SLOT[group[0]], len(group)
        vb = kv[1, lo:lo + n].reshape(n * keys, hd)
        dpbuf[lo:lo + n] = dot(vb, dot_b[...]).reshape(n, keys, rows)

    def softmax(group, first):
        lo, n = SLOT[group[0]], len(group)
        mx = top[lo:lo + 1]
        if first:
            m_new = mx
        else:
            m_old = m_ref[...]
            m_new = jnp.maximum(m_old, mx)
            alpha = jnp.exp2((m_old - m_new) * c2)
        m_ref[...] = m_new
        mc = m_new * c2
        total = None
        for i in range(n):
            p = jnp.exp2(sbuf[lo + i] * c2 - mc)
            pbuf[lo + i] = p.astype(jnp.bfloat16)
            part_sum = jnp.sum(p, axis=0, keepdims=True)
            total = part_sum if total is None else total + part_sum
        pv = dot(kv[1, lo:lo + n].reshape(n * keys, hd), pbuf[lo:lo + n].reshape(n * keys, rows), TN)
        if first:
            l_ref[...] = total
            o_t[...] = pv
        else:
            l_ref[...] = l_ref[...] * alpha + total
            o_t[...] = o_t[...] * alpha + pv

    def row_terms():
        m_fin, l_fin = m_ref[...], l_ref[...]
        has_key = m_fin > NEG * 0.5
        safe = jnp.where(has_key, l_fin, 1.0)
        o_b = jnp.where(has_key, o_t[...] / safe, 0.0).astype(jnp.bfloat16).astype(jnp.float32)
        o_t[...] = o_b
        delta_v[...] = jnp.sum(o_b * dot_t[...], axis=0, keepdims=True)
        lse_v[...] = jnp.where(has_key, m_fin * scale + jnp.log(safe), 0.0)
        lse2_v[...] = jnp.where(has_key, m_fin * c2 + jnp.log2(safe), 0.0)

    def rsend(X, a, b, o):
        step, key = target(X, a, b, o)
        i = RIDX[key]
        dev = nbr(unframe(X, *step), b == 0 and o == 1)
        push(part.at[X, SLOT[unframe(X, a, b)], o], rbuf.at[X, i], rs_send, rs_recv.at[X, RSEM[consumer(key)]], dev)

    def rwait(X, names):
        name = consumer(names[0])
        assert len(names) == RNUM[name]
        ref = rbuf.at[X, 0:len(names)]
        remote(ref, ref, rs_send, rs_recv.at[X, RSEM[name]], to_partner).wait_recv()
        return [rbuf[X, RIDX[key]] for key in names]

    def total(X, a, b, o):
        s = SLOT[unframe(X, a, b)]
        names = terms(X, a, b, o)
        if names:
            acc = part[X, s, o]
            for term in rwait(X, names):
                acc = acc + term
            part[X, s, o] = acc

    def backward(blk):
        s = SLOT[blk]
        p = jnp.exp2(sbuf[s] * c2 - lse2_v[...])
        pbuf[s] = p.astype(jnp.bfloat16)
        dsbuf[s] = (p * (dpbuf[s] - delta_v[...])).astype(jnp.bfloat16)
        part[1, s] = dot(pbuf[s], dob[...].reshape(rows, hd)).reshape(CORES, tok, hd)
        part[0, s] = dot(dsbuf[s], qbuf[...].reshape(rows, hd)).reshape(CORES, tok, hd)

    x_out, x_lse = [], []

    local = []

    def store(src, dst, i):
        c = pltpu.make_async_copy(src, dst, loc_sem.at[i])
        c.start()
        local.append(c)

    def store_o():
        ost[...] = jnp.transpose(o_t[...]).astype(jnp.bfloat16).reshape(2 * grp, tok, hd)
        for i in range(CORES):
            for h in range(grp):
                j = (i * grp + h) * tok
                lsest[i, h:h + 1, :] = lse_v[:, j:j + tok]
        store(ost.at[0:grp], o_out.at[pl.ds(mine, grp)], 0)
        x_out.append(push(ost.at[grp:2 * grp], o_out.at[pl.ds(mine, grp)], pair_send.at[0], pair_recv.at[2], to_partner))
        x_lse.append(push(lsest.at[1], lsest.at[2], pair_send.at[1], pair_recv.at[3], to_partner))

    def store_dq():
        dq_t = dot(kaug[:, :, 0:hd].reshape(NBLK * keys, hd), dsbuf[...].reshape(NBLK * keys, rows), TN)
        dqst[...] = (jnp.transpose(dq_t) * scale).astype(jnp.bfloat16).reshape(2 * grp, tok, hd)
        store(dqst.at[0:grp], dq_out.at[pl.ds(mine, grp)], 1)
        x_out.append(push(dqst.at[grp:2 * grp], dq_out.at[pl.ds(mine, grp)], pair_send.at[0], pair_recv.at[2], to_partner))

    def finish(X, o):
        total(X, 0, 0, o)
        if o == 1:
            key = ('lo', 1)
            push(part.at[X, 0, 1], rbuf.at[X, RIDX[key]], rs_send, rs_recv.at[X, RSEM[consumer(key)]], to_partner)
        else:
            grad[X, 0] = part[X, 0, 0] * scale if X == 0 else part[X, 0, 0]

    def finish_other(X):
        acc = sum(rwait(X, (('lo', 1), ('fa', 1, 1), ('fa', 1, -1), ('ra', 1))))
        grad[X, 1] = acc * scale if X == 0 else acc

    def need_q():
        if 'q' not in ready:
            ready.add('q')
            c_q.wait()
            x_q.wait_recv()
            qt[0:hd, :] = jnp.transpose(qbuf[...].reshape(rows, hd).astype(jnp.float32)).astype(jnp.bfloat16)

    def need_do():
        if 'do' not in ready:
            ready.add('do')
            c_do.wait()
            x_do.wait_recv()
            do_t = jnp.transpose(dob[...].reshape(rows, hd).astype(jnp.float32))
            dot_t[...] = do_t
            dot_b[...] = do_t.astype(jnp.bfloat16)

    def group_part(gi, stage):
        group = GROUPS[gi]
        first = stage not in ready
        ready.add(stage)
        with scope('wait%d_%d' % (gi, stage)):
            for blk in group:
                for o in range(CORES):
                    arrive(min(stage, 1), blk, o)
            if stage == 0:
                need_q()
            elif stage == 2:
                need_do()
        with scope('group%d_%d' % (gi, stage)):
            if stage == 0:
                scores(group)
            elif stage == 1:
                softmax(group, first)
            else:
                grads_p(group)

    def pass_on(X, a, b, o):
        if (a, b) == (0, 0):
            finish(X, o)
        else:
            total(X, a, b, o)
            rsend(X, a, b, o)

    ready = set()
    for code, *item in ORDER[early:]:
        with scope('%d_' % code + '_'.join(map(str, item))):
            if code == 0:
                forward(*item)
            elif code == 1:
                group_part(*item)
            elif code == 2:
                need_do()
                row_terms()
            elif code == 3:
                backward(tuple(item))
            elif code == 4:
                pass_on(*item)
            elif code == 5:
                (store_o, store_dq)[item[0]]()
            else:
                finish_other(*item)

    scope_out = scope('tail')
    scope_out.__enter__()
    x_lse[0].wait_recv()
    lse_all[0:grp] = jnp.where(core == 0, lsest[0], lsest[2])
    lse_all[grp:2 * grp] = jnp.where(core == 0, lsest[2], lsest[0])
    store(lse_all, lse_out, 4)
    for X, out in ((0, dk_out), (1, dv_out)):
        own, other = grad[X, 0], grad[X, 1]
        tmp32[X, pl.ds(0, tok, stride=2), :] = jnp.where(core == 0, own, other)
        tmp32[X, pl.ds(1, tok, stride=2), :] = jnp.where(core == 0, other, own)
        outb[X] = tmp32[X].astype(jnp.bfloat16)
        store(outb.at[X], out, 2 + X)
    for ref, sem in ((rbuf.at[0], ag_send), (rbuf, rs_send), (dpbuf.at[0], pair_send.at[0])):
        remote(ref, ref, sem, sem, to_partner).wait_send()
    x_lse[0].wait_send()
    remote(ost, ost, pair_send.at[0], pair_recv.at[2], to_partner).wait_recv()
    for c in local:
        c.wait()
    scope_out.__exit__(None, None, None)


def store_kernel(*refs):
    n = len(refs) // 2
    copies = [pltpu.make_async_copy(refs[i], refs[n + i], refs[-1].at[i]) for i in range(n)]
    for c in copies:
        c.start()
    for c in copies:
        c.wait()


def solution(mesh):
    cp = mesh.shape['cp']
    tok_spec = P(('dp', 'cp'), None, None)

    def local(q, k, v, do, valid, cu):
        tok, heads, hd = q.shape
        kvh = k.shape[1]
        grp = heads // kvh
        n_docs = cu.shape[0] - 1
        rows = CORES * grp * tok
        keys = CORES * tok
        assert kvh == CORES and cp == CORES * SIDE * SIDE and keys == hd
        bf, f32 = jnp.bfloat16, jnp.float32
        hbm_spec = pl.BlockSpec(memory_space=pltpu.HBM)
        any_spec = pl.BlockSpec(memory_space=pl.ANY)
        n_rs = len(RIDX)
        flat = lambda x: x.reshape(tok * kvh, hd)
        o, lse, dq, dk, dv = pl.pallas_call(
            functools.partial(kernel, cp, n_docs, hd ** -0.5),
            name='ring_attention',
            out_shape=[
                jax.ShapeDtypeStruct((heads, tok, hd), bf),
                jax.ShapeDtypeStruct((heads, tok), f32),
                jax.ShapeDtypeStruct((heads, tok, hd), bf),
                jax.ShapeDtypeStruct((tok * kvh, hd), bf),
                jax.ShapeDtypeStruct((tok * kvh, hd), bf),
            ],
            in_specs=[hbm_spec] * 6,
            out_specs=[any_spec] * 5,
            scratch_shapes=[
                pltpu.VMEM((2, tok * kvh, hd), bf),
                pltpu.VMEM((2, tok * kvh, hd), f32),
                pltpu.VMEM((2, tok, hd), bf),
                pltpu.VMEM((2, NBLK, CORES, tok, hd), bf),
                pltpu.VMEM((NBLK, keys, 2 * hd), bf),
                pltpu.VMEM((CORES * grp, tok, hd), bf),
                pltpu.VMEM((hd + keys, rows), bf),
                pltpu.VMEM((CORES * grp, tok, hd), bf),
                pltpu.VMEM((hd, rows), f32),
                pltpu.VMEM((hd, rows), bf),
                pltpu.VMEM((NBLK, keys, rows), f32),
                pltpu.VMEM((NBLK, keys, rows), f32),
                pltpu.VMEM((NBLK, keys, rows), bf),
                pltpu.VMEM((NBLK, keys, rows), bf),
                pltpu.VMEM((2, NBLK, CORES, tok, hd), f32),
                pltpu.VMEM((2, n_rs, tok, hd), f32),
                pltpu.VMEM((heads, tok, hd), bf),
                pltpu.VMEM((heads, tok, hd), bf),
                pltpu.VMEM((CORES + 1, grp, tok), f32),
                pltpu.VMEM((2, 2, tok, hd), f32),
                pltpu.VMEM((2, tok * kvh, hd), f32),
                pltpu.VMEM((2, tok * kvh, hd), bf),
                pltpu.VMEM((heads, tok), f32),
                pltpu.VMEM((1, rows), f32),
                pltpu.VMEM((1, rows), f32),
                pltpu.VMEM((1, rows), f32),
                pltpu.VMEM((1, rows), f32),
                pltpu.VMEM((1, rows), f32),
                pltpu.VMEM((NBLK, rows), f32),
                pltpu.VMEM((hd, rows), f32),
                pltpu.VMEM((1, tok), jnp.int32),
                pltpu.SMEM((1, n_docs + 1), jnp.int32),
                pltpu.SemaphoreType.DMA((5,)),
                pltpu.SemaphoreType.DMA((2,)),
                pltpu.SemaphoreType.DMA((4,)),
                pltpu.SemaphoreType.DMA(()),
                pltpu.SemaphoreType.DMA((len(AIDX),)),
                pltpu.SemaphoreType.DMA(()),
                pltpu.SemaphoreType.DMA((2, len(RSEM))),
            ],
            compiler_params=pltpu.CompilerParams(
                collective_id=0, has_side_effects=True, vmem_limit_bytes=40 * 1024 * 1024),
        )(*(pltpu.with_memory_space_constraint(a, pltpu.HBM) for a in (q.transpose(1, 0, 2), flat(k), flat(v), do.transpose(1, 0, 2), valid.reshape(1, tok), cu.reshape(1, n_docs + 1))))
        o, lse, dq, dk, dv = pl.pallas_call(
            store_kernel,
            name='store_outputs',
            out_shape=[
                jax.ShapeDtypeStruct((heads, tok, hd), bf),
                jax.ShapeDtypeStruct((heads, tok), f32),
                jax.ShapeDtypeStruct((heads, tok, hd), bf),
                jax.ShapeDtypeStruct((tok * kvh, hd), bf),
                jax.ShapeDtypeStruct((tok * kvh, hd), bf),
            ],
            in_specs=[any_spec] * 5,
            out_specs=[hbm_spec] * 5,
            scratch_shapes=[pltpu.SemaphoreType.DMA((5,))],
            compiler_params=pltpu.CompilerParams(vmem_limit_bytes=1024 * 1024),
        )(o, lse, dq, dk, dv)
        back = lambda x: x.reshape(tok, kvh, hd)
        return (o.transpose(1, 0, 2), lse.transpose(1, 0), dq.transpose(1, 0, 2), back(dk), back(dv))

    return jax.shard_map(
        local, mesh=mesh,
        in_specs=(tok_spec, tok_spec, tok_spec, tok_spec, P(('dp', 'cp')), P('dp')),
        out_specs=(tok_spec, P(('dp', 'cp'), None), tok_spec, tok_spec, tok_spec), check_vma=False)
```
